32 devices in a mesh: dp: 1 (over z), cfg: 4 (over y), tp: 8 (over x, core).
Axes of the slice: x: 4, y: 4, z: 1, core: 2. Of those that a mesh axis runs over, the one named last changes fastest.
The devices are a block of a 4x4x8 slice.
Arguments:
- hidden: bfloat16 [4, 4096, 1152], P(('dp', 'cfg'))
- caption: bfloat16 [4, 300, 1152], P(('dp', 'cfg'))
- cap_len: int32 [4], P(('dp', 'cfg'))
- t_block: bfloat16 [2, 6912], P('dp')
- t_embed: bfloat16 [2, 1152], P('dp')
- x_t: float32 [2, 128, 128, 4], P('dp')
- alpha_bar: float32 [2, 2], P('dp')
- mod_table: bfloat16 [2, 6, 1152], replicated
- w_qkv: bfloat16 [2, 1152, 3, 16, 72], P(None, None, None, 'tp')
- w_proj: bfloat16 [2, 16, 72, 1152], P(None, 'tp')
- w_cq: bfloat16 [2, 1152, 16, 72], P(None, None, 'tp')
- w_ckv: bfloat16 [2, 1152, 2, 16, 72], P(None, None, None, 'tp')
- w_cproj: bfloat16 [2, 16, 72, 1152], P(None, 'tp')
- w_fc1: bfloat16 [2, 1152, 4608], P(None, None, 'tp')
- w_fc2: bfloat16 [2, 4608, 1152], P(None, 'tp')
- final_table: bfloat16 [2, 1152], replicated
- w_out: bfloat16 [1152, 32], replicated
- b_out: bfloat16 [32], replicated
Outputs:
- output: float32 [2, 128, 128, 4], P('dp')
All inputs are finite; a program needn't handle non-finite values.
Results may differ from the reference program's by a relative error of at most 0.013431.
Values are sent between devices in bfloat16 or wider.
A program may use at most 768 MiB of HBM per device.

```python
import jax
import jax.numpy as jnp
from jax import lax

BATCH_SIZE = 2
LATENT_SIDE = 128
MODEL_DIM = 1152
NUM_HEADS = 16
TEXT_LEN = 300
HIDDEN_FF = 4608

NUM_TOKENS = (LATENT_SIDE // 2) * (LATENT_SIDE // 2)
HEAD_DIM = MODEL_DIM // NUM_HEADS
GUIDANCE = 4.5
LN_EPS = 1e-6


def setup_inputs(seed: int = 0, part: int = 0) -> dict:
    part_keys = jax.random.split(jax.random.fold_in(jax.random.key(seed), part), 10)
    weight_keys = jax.random.split(jax.random.key(seed + 1), 11)
    total_rows = 2 * BATCH_SIZE
    common = jax.random.normal(part_keys[0], (total_rows, 1, MODEL_DIM), jnp.float32)
    tok_noise = jax.random.normal(part_keys[1], (total_rows, NUM_TOKENS, MODEL_DIM), jnp.float32)
    hidden = common + tok_noise
    cap_mean = jax.random.normal(part_keys[2], (total_rows, 1, MODEL_DIM), jnp.float32)
    caption = cap_mean + jax.random.normal(part_keys[3], (total_rows, TEXT_LEN, MODEL_DIM), jnp.float32)
    len_keys = jax.random.split(part_keys[4], 2)
    cond_len = jax.random.randint(len_keys[0], (BATCH_SIZE,), TEXT_LEN // 4, TEXT_LEN + 1)
    uncond_len = jax.random.randint(len_keys[1], (BATCH_SIZE,), 1, TEXT_LEN // 16 + 2)
    cap_len = jnp.concatenate([cond_len.at[0].set(TEXT_LEN), uncond_len]).astype(jnp.int32)
    t_block = 0.5 * jax.random.normal(part_keys[5], (BATCH_SIZE, 6 * MODEL_DIM), jnp.float32)
    t_embed = 0.5 * jax.random.normal(part_keys[6], (BATCH_SIZE, MODEL_DIM), jnp.float32)
    x_t = jax.random.normal(part_keys[7], (BATCH_SIZE, LATENT_SIDE, LATENT_SIDE, 4), jnp.float32)
    abar_t = jax.random.uniform(part_keys[8], (BATCH_SIZE,), jnp.float32, 0.15, 0.6)
    abar_gap = jax.random.uniform(part_keys[9], (BATCH_SIZE,), jnp.float32, 0.1, 0.3)
    alpha_bar = jnp.stack([abar_t, abar_t + abar_gap], axis=1)
    dim_scale = MODEL_DIM ** -0.5
    ff_scale = HIDDEN_FF ** -0.5
    mod_table = 0.5 * jax.random.normal(weight_keys[0], (2, 6, MODEL_DIM), jnp.float32)
    w_qkv = dim_scale * jax.random.normal(weight_keys[1], (2, MODEL_DIM, 3, NUM_HEADS, HEAD_DIM), jnp.float32)
    w_proj = dim_scale * jax.random.normal(weight_keys[2], (2, NUM_HEADS, HEAD_DIM, MODEL_DIM), jnp.float32)
    w_cq = dim_scale * jax.random.normal(weight_keys[3], (2, MODEL_DIM, NUM_HEADS, HEAD_DIM), jnp.float32)
    w_ckv = dim_scale * jax.random.normal(weight_keys[4], (2, MODEL_DIM, 2, NUM_HEADS, HEAD_DIM), jnp.float32)
    w_cproj = dim_scale * jax.random.normal(weight_keys[5], (2, NUM_HEADS, HEAD_DIM, MODEL_DIM), jnp.float32)
    w_fc1 = dim_scale * jax.random.normal(weight_keys[6], (2, MODEL_DIM, HIDDEN_FF), jnp.float32)
    w_fc2 = ff_scale * jax.random.normal(weight_keys[7], (2, HIDDEN_FF, MODEL_DIM), jnp.float32)
    final_table = 0.5 * jax.random.normal(weight_keys[8], (2, MODEL_DIM), jnp.float32)
    w_out = dim_scale * jax.random.normal(weight_keys[9], (MODEL_DIM, 32), jnp.float32)
    b_out = 0.3 * jax.random.normal(weight_keys[10], (32,), jnp.float32)
    return {
        'hidden': hidden.astype(jnp.bfloat16),
        'caption': caption.astype(jnp.bfloat16),
        'cap_len': cap_len,
        't_block': t_block.astype(jnp.bfloat16),
        't_embed': t_embed.astype(jnp.bfloat16),
        'x_t': x_t,
        'alpha_bar': alpha_bar,
        'mod_table': mod_table.astype(jnp.bfloat16),
        'w_qkv': w_qkv.astype(jnp.bfloat16),
        'w_proj': w_proj.astype(jnp.bfloat16),
        'w_cq': w_cq.astype(jnp.bfloat16),
        'w_ckv': w_ckv.astype(jnp.bfloat16),
        'w_cproj': w_cproj.astype(jnp.bfloat16),
        'w_fc1': w_fc1.astype(jnp.bfloat16),
        'w_fc2': w_fc2.astype(jnp.bfloat16),
        'final_table': final_table.astype(jnp.bfloat16),
        'w_out': w_out.astype(jnp.bfloat16),
        'b_out': b_out.astype(jnp.bfloat16),
    }


def layer_norm(values):
    mean_val = jnp.mean(values, axis=-1, keepdims=True)
    centered = values - mean_val
    variance = jnp.mean(centered * centered, axis=-1, keepdims=True)
    return centered * lax.rsqrt(variance + LN_EPS)


def attend(queries, key_vecs, values, key_mask):
    def one_head(head_in):
        q_head, k_head, v_head = head_in
        scores = jnp.dot(q_head, k_head.T, preferred_element_type=jnp.float32) * HEAD_DIM ** -0.5
        scores = jnp.where(key_mask[None, :], scores, -1e30)
        attn_prob = jax.nn.softmax(scores, axis=-1).astype(jnp.bfloat16)
        return jnp.dot(attn_prob, v_head, preferred_element_type=jnp.float32).astype(jnp.bfloat16)
    per_head = lax.map(one_head, (jnp.swapaxes(queries, 0, 1), jnp.swapaxes(key_vecs, 0, 1), jnp.swapaxes(values, 0, 1)))
    return jnp.swapaxes(per_head, 0, 1)


def block_row(residual, caption_row, key_mask, t_mods, layer_w):
    mod_tab, w_qkv, w_proj, w_cq, w_ckv, w_cproj, w_fc1, w_fc2 = layer_w
    mod_rows = mod_tab.astype(jnp.float32) + t_mods
    all_keys = jnp.ones((NUM_TOKENS,), jnp.bool_)
    attn_in = (layer_norm(residual) * (1.0 + mod_rows[1]) + mod_rows[0]).astype(jnp.bfloat16)
    qkv_out = jnp.dot(attn_in, w_qkv.reshape(MODEL_DIM, 3 * MODEL_DIM), preferred_element_type=jnp.float32)
    qkv_out = qkv_out.astype(jnp.bfloat16).reshape(NUM_TOKENS, 3, NUM_HEADS, HEAD_DIM)
    self_o = attend(qkv_out[:, 0], qkv_out[:, 1], qkv_out[:, 2], all_keys)
    self_proj = jnp.dot(self_o.reshape(NUM_TOKENS, MODEL_DIM), w_proj.reshape(MODEL_DIM, MODEL_DIM), preferred_element_type=jnp.float32).astype(jnp.bfloat16)
    residual = residual + mod_rows[2] * self_proj.astype(jnp.float32)
    cross_q = jnp.dot(residual.astype(jnp.bfloat16), w_cq.reshape(MODEL_DIM, MODEL_DIM), preferred_element_type=jnp.float32)
    cross_q = cross_q.astype(jnp.bfloat16).reshape(NUM_TOKENS, NUM_HEADS, HEAD_DIM)
    cross_kv = jnp.dot(caption_row, w_ckv.reshape(MODEL_DIM, 2 * MODEL_DIM), preferred_element_type=jnp.float32)
    cross_kv = cross_kv.astype(jnp.bfloat16).reshape(TEXT_LEN, 2, NUM_HEADS, HEAD_DIM)
    cross_o = attend(cross_q, cross_kv[:, 0], cross_kv[:, 1], key_mask)
    cross_proj = jnp.dot(cross_o.reshape(NUM_TOKENS, MODEL_DIM), w_cproj.reshape(MODEL_DIM, MODEL_DIM), preferred_element_type=jnp.float32).astype(jnp.bfloat16)
    residual = residual + cross_proj.astype(jnp.float32)
    mlp_in = (layer_norm(residual) * (1.0 + mod_rows[4]) + mod_rows[3]).astype(jnp.bfloat16)
    mlp_hidden = jax.nn.gelu(jnp.dot(mlp_in, w_fc1, preferred_element_type=jnp.float32), approximate=True).astype(jnp.bfloat16)
    mlp_out = jnp.dot(mlp_hidden, w_fc2, preferred_element_type=jnp.float32).astype(jnp.bfloat16)
    return residual + mod_rows[5] * mlp_out.astype(jnp.float32)


def reference(hidden, caption, cap_len, t_block, t_embed, x_t, alpha_bar, mod_table, w_qkv, w_proj, w_cq, w_ckv, w_cproj, w_fc1, w_fc2, final_table, w_out, b_out):
    t_rows = jnp.tile(t_block.astype(jnp.float32).reshape(BATCH_SIZE, 6, MODEL_DIM), (2, 1, 1))
    emb_rows = jnp.tile(t_embed.astype(jnp.float32), (2, 1))
    layer_ws = (mod_table, w_qkv, w_proj, w_cq, w_ckv, w_cproj, w_fc1, w_fc2)

    def per_row(row_in):
        hidden_row, caption_row, len_row, t_mods, emb_row = row_in
        key_mask = jnp.arange(TEXT_LEN) < len_row

        def layer_step(residual, layer_w):
            return block_row(residual, caption_row, key_mask, t_mods, layer_w), None

        residual, scan_out = lax.scan(layer_step, hidden_row.astype(jnp.float32), layer_ws)
        shift_scale = final_table.astype(jnp.float32) + emb_row[None, :]
        final_in = (layer_norm(residual) * (1.0 + shift_scale[1]) + shift_scale[0]).astype(jnp.bfloat16)
        out_tok = jnp.dot(final_in, w_out, preferred_element_type=jnp.float32) + b_out.astype(jnp.float32)
        grid_side = LATENT_SIDE // 2
        patches = out_tok.reshape(grid_side, grid_side, 2, 2, 8)[:, :, :, :, :4]
        return patches.transpose(0, 2, 1, 3, 4).reshape(LATENT_SIDE, LATENT_SIDE, 4)

    eps_rows = lax.map(per_row, (hidden, caption, cap_len, t_rows, emb_rows))
    eps_cond = eps_rows[:BATCH_SIZE]
    eps_uncond = eps_rows[BATCH_SIZE:]
    guided = eps_uncond + GUIDANCE * (eps_cond - eps_uncond)
    abar_t = alpha_bar[:, 0][:, None, None, None]
    abar_prev = alpha_bar[:, 1][:, None, None, None]
    x_zero = (x_t - jnp.sqrt(1.0 - abar_t) * guided) / jnp.sqrt(abar_t)
    return jnp.sqrt(abar_prev) * x_zero + jnp.sqrt(1.0 - abar_prev) * guided
```

```python
import functools

import jax
import jax.numpy as jnp
from jax import lax
from jax.experimental import pallas as pl
from jax.experimental.pallas import tpu as pltpu
from jax.sharding import PartitionSpec as P

GUIDANCE = 4.5
LN_EPS = 1e-6
LOG2E = 1.4426950408889634
NT = (((1,), (1,)), ((), ()))
BF = jnp.bfloat16
F32 = jnp.float32


def layer_norm(values):
    mean_val = jnp.mean(values, axis=-1, keepdims=True)
    centered = values - mean_val
    variance = jnp.mean(centered * centered, axis=-1, keepdims=True)
    return centered * lax.rsqrt(variance + LN_EPS)


def dot(a, b):
    return jnp.dot(a, b, preferred_element_type=F32)


def dot_nt(a, b):
    return lax.dot_general(a, b, NT, preferred_element_type=F32)


def attn_kernel(cfg, src_ref, mod_ref, w_ref, o_ref, x_vm, q_vm, k_vm, vt_vm, s0, s1, sems):
    n_tok, n_dest, heads, hd, tok_blk, qb, kb, use_ln = cfg
    n_blk = n_tok // tok_blk
    hw = heads * hd
    scale = hd ** -0.5 * LOG2E

    def load(i):
        rows = pl.ds(pl.multiple_of(i * tok_blk, tok_blk), tok_blk)
        return pltpu.make_async_copy(src_ref.at[rows], x_vm.at[rows], sems.at[i])

    for i in range(n_blk):
        load(i).start()
    row_id = lax.broadcasted_iota(jnp.int32, (80 - hd, n_tok), 0)
    for h in range(heads):
        vt_vm[h, hd:, :] = jnp.where(row_id == 0, 1.0, 0.0).astype(BF)

    def qkv_step(i, carry):
        load(i).wait()
        rows = pl.ds(pl.multiple_of(i * tok_blk, tok_blk), tok_blk)
        x = x_vm[rows, :]
        if use_ln:
            x = (layer_norm(x.astype(F32)) * (1.0 + mod_ref[1:2, :]) + mod_ref[0:1, :]).astype(BF)
        qkv = dot(x, w_ref[...])
        q = qkv[:, :hw] * scale
        lane = lax.broadcasted_iota(jnp.int32, q.shape, 1)
        for h in range(heads):
            q_vm[h, rows, :] = jnp.where((lane >= h * hd) & (lane < (h + 1) * hd), q, 0.0).astype(BF)
        k_vm[rows, :] = qkv[:, hw:2 * hw].astype(BF)
        vt = qkv[:, 2 * hw:].T
        for h in range(heads):
            vt_vm[h, :hd, rows] = vt[h * hd:(h + 1) * hd, :].astype(BF)
        return carry

    lax.fori_loop(0, n_blk, qkv_step, 0)

    bufs = (s0, s1)
    n_kb = n_tok // kb
    dest_tok = n_tok // n_dest

    def q_step(i, carry):
        h = lax.rem(i, heads)
        qi = lax.div(i, heads)
        q = q_vm[h, pl.ds(pl.multiple_of(qi * qb, qb), qb), :]

        def scores(j, dst):
            s = dot_nt(k_vm[j * kb:(j + 1) * kb, :], q)
            dst[...] = s
            return jnp.max(jnp.max(s.reshape(kb // 8, 8, qb), axis=0), axis=0, keepdims=True)

        m = scores(0, bufs[0])
        acc = None
        for j in range(n_kb):
            blk_max = scores(j + 1, bufs[(j + 1) % 2]) if j + 1 < n_kb else None
            p = jnp.exp2(bufs[j % 2][...] - m).astype(BF)
            pv = dot(vt_vm[h, :, j * kb:(j + 1) * kb], p)
            acc = pv if acc is None else acc + pv
            if blk_max is not None:
                m_new = jnp.maximum(m, blk_max)
                acc = acc * jnp.exp2(m - m_new)
                m = m_new
        o = (acc[:hd] / acc[hd:hd + 1]).astype(BF)
        for u in range(qb // dest_tok):
            o_ref[qi * (qb // dest_tok) + u, h, :, :] = o[:, u * dest_tok:(u + 1) * dest_tok]
        return carry

    lax.fori_loop(0, heads * (n_tok // qb), q_step, 0)


def self_attention(src, mods, w, n_dest, heads, hd, use_ln):
    n_tok, dim = src.shape
    tok_blk, qb, kb = 512, 1024, 512
    cfg = (n_tok, n_dest, heads, hd, tok_blk, qb, kb, use_ln)
    vmem = pl.BlockSpec(memory_space=pltpu.VMEM)
    return pl.pallas_call(
        functools.partial(attn_kernel, cfg),
        out_shape=jax.ShapeDtypeStruct((n_dest, heads, hd, n_tok // n_dest), BF),
        in_specs=[pl.BlockSpec(memory_space=pl.ANY), vmem, vmem],
        out_specs=vmem,
        scratch_shapes=[
            pltpu.VMEM((n_tok, dim), BF),
            pltpu.VMEM((heads, n_tok, heads * hd), BF),
            pltpu.VMEM((n_tok, heads * hd), BF),
            pltpu.VMEM((heads, 80, n_tok), BF),
            pltpu.VMEM((kb, qb), F32),
            pltpu.VMEM((kb, qb), F32),
            pltpu.SemaphoreType.DMA((n_tok // tok_blk,)),
        ],
        compiler_params=pltpu.CompilerParams(vmem_limit_bytes=60 << 20),
        cost_estimate=pl.CostEstimate(flops=30 * 10 ** 9, bytes_accessed=20 * 10 ** 6, transcendentals=0),
    )(src, mods, w)


def tok_kernel(cfg, o_ref, x_ref, g_ref, kc_ref, vc_ref, mod_ref, wo_ref, bo_ref, *refs):
    tp, hd, rows_p, rows_f, last = cfg
    if last:
        (e_ref, wp, wcp, wcq, w1, w2, x_vm, h_vm, q_vm, sems, xsem) = refs
    else:
        (xo_ref, a_ref, wp, wcp, wcq, w1, w2, x_vm, h_vm, q_vm, sems, xsem) = refs
    n_tok, dim = x_vm.shape
    n_heads = o_ref.shape[0] * o_ref.shape[1]
    scale = hd ** -0.5 * LOG2E
    mats = ((wp, rows_p), (wcp, rows_p), (wcq, rows_p), (w1, rows_f), (w2, rows_f))

    def copies(which):
        off = sum(r for _, r in mats[:which])
        dst, rows = mats[which]
        return [pltpu.make_async_copy(g_ref.at[t, pl.ds(off, rows)], dst.at[pl.ds(t * rows, rows)], sems.at[which, t])
                for t in range(tp)]

    if x_ref.shape[0] == n_tok:
        x_src = x_ref
    else:
        x_src = x_ref.at[pl.ds(pl.multiple_of(lax.axis_index("tp") * n_tok, n_tok), n_tok)]
    x_copy = pltpu.make_async_copy(x_src, x_vm, xsem)
    x_copy.start()
    for which in (0, 2, 1, 3, 4):
        for c in copies(which):
            c.start()

    def ready(which):
        for c in copies(which):
            c.wait()

    def mod(i):
        return mod_ref[i:i + 1, :]

    def stack_t(parts):
        return jnp.concatenate(parts, axis=0).T.astype(BF)

    o = stack_t([o_ref[t, h].astype(F32) for t in range(o_ref.shape[0]) for h in range(o_ref.shape[1])])
    ready(0)
    proj = dot(o, wp[...]).astype(BF).astype(F32)
    x_copy.wait()
    x1 = x_vm[...].astype(F32) + mod(2) * proj
    ready(2)
    qt = (dot_nt(x1.astype(BF), wcq[...]) * scale).T
    pad_row = lax.broadcasted_iota(jnp.int32, (80 - hd, n_tok), 0)
    ones_row = jnp.where(pad_row == 0, 1.0, 0.0).astype(BF)
    for h in range(n_heads):
        q_vm[h, :hd, :] = qt[h * hd:(h + 1) * hd, :].astype(BF)
        q_vm[h, hd:, :] = ones_row
    outs = []
    for h in range(n_heads):
        s = dot(kc_ref[h], q_vm[h])
        p = jnp.exp2(s - jnp.max(s, axis=0, keepdims=True)).astype(BF)
        pv = dot(vc_ref[h], p)
        outs.append(pv[:hd] / pv[hd:hd + 1])
    oc = stack_t([v.astype(BF).astype(F32) for v in outs])
    ready(1)
    x2 = x1 + dot(oc, wcp[...]).astype(BF).astype(F32)
    a2 = (layer_norm(x2) * (1.0 + mod(4)) + mod(3)).astype(BF)
    ready(3)
    n_ff = w1.shape[0]
    step = n_ff // 3
    for j in range(3):
        h_vm[:, j * step:(j + 1) * step] = jax.nn.gelu(dot_nt(a2, w1[j * step:(j + 1) * step, :]), approximate=True).astype(BF)
    ready(4)
    x3 = x2 + mod(5) * dot(h_vm[...], w2[...]).astype(BF).astype(F32)
    a = (layer_norm(x3) * (1.0 + mod(7)) + mod(6)).astype(BF)
    if last:
        e_ref[...] = dot(a, wo_ref[...]) + bo_ref[...]
    else:
        xo_ref[...] = x3
        a_ref[...] = a


def token_block(o, x, gathered, kc, vc, mods, w_out, b_out, last):
    tp, n_src_heads, hd, n_tok = o.shape
    dim = x.shape[1]
    rows_p = n_src_heads * hd
    rows_f = (gathered.shape[1] - 3 * rows_p) // 2
    cfg = (tp, hd, rows_p, rows_f, last)
    vmem = pl.BlockSpec(memory_space=pltpu.VMEM)
    hbm = pl.BlockSpec(memory_space=pl.ANY)
    if last:
        out_shape = jax.ShapeDtypeStruct((n_tok, w_out.shape[1]), F32)
        out_specs = vmem
    else:
        out_shape = (jax.ShapeDtypeStruct((n_tok, dim), F32), jax.ShapeDtypeStruct((n_tok, dim), BF))
        out_specs = (vmem, vmem)
    return pl.pallas_call(
        functools.partial(tok_kernel, cfg),
        out_shape=out_shape,
        in_specs=[vmem, hbm, hbm, vmem, vmem, vmem, vmem, vmem],
        out_specs=out_specs,
        scratch_shapes=[
            pltpu.VMEM((tp * rows_p, dim), BF),
            pltpu.VMEM((tp * rows_p, dim), BF),
            pltpu.VMEM((tp * rows_p, dim), BF),
            pltpu.VMEM((tp * rows_f, dim), BF),
            pltpu.VMEM((tp * rows_f, dim), BF),
            pltpu.VMEM((n_tok, dim), x.dtype),
            pltpu.VMEM((n_tok, tp * rows_f), BF),
            pltpu.VMEM((tp * n_src_heads, 80, n_tok), BF),
            pltpu.SemaphoreType.DMA((5, tp)),
            pltpu.SemaphoreType.DMA,
        ],
        compiler_params=pltpu.CompilerParams(vmem_limit_bytes=63 << 20),
        cost_estimate=pl.CostEstimate(flops=20 * 10 ** 9, bytes_accessed=40 * 10 ** 6, transcendentals=0),
    )(o, x, gathered, kc, vc, mods, w_out, b_out)


def solution(mesh):
    row_spec = P(('dp', 'cfg'))
    part_spec = P('dp')
    in_specs = (row_spec, row_spec, row_spec, part_spec, part_spec, part_spec, part_spec, P(),
                P(None, None, None, 'tp'), P(None, 'tp'), P(None, None, 'tp'), P(None, None, None, 'tp'),
                P(None, 'tp'), P(None, None, 'tp'), P(None, 'tp'), P(), P(), P())
    tp = mesh.shape['tp']
    n_cfg = mesh.shape['cfg']

    def local_step(hidden, caption, cap_len, t_block, t_embed, x_t, alpha_bar, mod_table, w_qkv, w_proj, w_cq, w_ckv, w_cproj, w_fc1, w_fc2, final_table, w_out, b_out):
        n_tok, dim = hidden.shape[1:]
        n_layers, _, _, heads, hd = w_qkv.shape
        hw = heads * hd
        row_start = lax.axis_index('cfg') % t_block.shape[0]
        t_rows = lax.dynamic_slice_in_dim(t_block, row_start, 1, axis=0).astype(F32).reshape(6, dim)
        emb = lax.dynamic_slice_in_dim(t_embed, row_start, 1, axis=0).astype(F32)
        fin = final_table.astype(F32) + emb
        mods = [mod_table[l].astype(F32) + t_rows for l in range(n_layers)]
        n_cap = caption.shape[1]
        cap_pad = -(-n_cap // 8) * 8
        key_id = jnp.arange(cap_pad)
        bias = jnp.where(key_id < jnp.minimum(cap_len[0], n_cap), 0.0, -1e30).astype(BF)

        packs, kcs, vcs = [], [], []
        for l in range(n_layers):
            packs.append(jnp.concatenate([
                w_proj[l].reshape(hw, dim), w_cproj[l].reshape(hw, dim), w_cq[l].reshape(dim, hw).T,
                w_fc1[l].T, w_fc2[l]], axis=0))
        gath = [lax.all_gather(p, 'tp', axis=0) for p in packs]
        cap = jnp.pad(caption[0], ((0, cap_pad - n_cap), (0, 0)))
        for l in range(n_layers):
            kv = dot(cap, w_ckv[l].reshape(dim, 2 * hw)).astype(BF)
            kv = lax.all_gather(kv, 'tp', axis=0).reshape(tp, cap_pad, 2, heads, hd)
            k = kv[:, :, 0].transpose(0, 2, 1, 3).reshape(tp * heads, cap_pad, hd)
            k = jnp.concatenate([k, jnp.broadcast_to(bias[None, :, None], (tp * heads, cap_pad, 1)),
                                 jnp.zeros((tp * heads, cap_pad, 80 - hd - 1), BF)], axis=2)
            v = kv[:, :, 1].transpose(0, 2, 3, 1).reshape(tp * heads, hd, cap_pad)
            v = jnp.concatenate([v, jnp.ones((tp * heads, 1, cap_pad), BF), jnp.zeros((tp * heads, 80 - hd - 1, cap_pad), BF)], axis=1)
            kcs.append(k)
            vcs.append(v)

        n_ch = w_out.shape[1] // 4
        keep = n_ch // 2
        w16 = w_out.reshape(dim, 4, n_ch)[:, :, :keep].reshape(dim, 4 * keep)
        w16 = jnp.pad(w16, ((0, 0), (0, 128 - 4 * keep)))
        b16 = jnp.pad(b_out.astype(F32).reshape(4, n_ch)[:, :keep].reshape(1, 4 * keep), ((0, 0), (0, 128 - 4 * keep)))

        src = hidden[0]
        x = src
        for l in range(n_layers):
            o = self_attention(src, mods[l], w_qkv[l].reshape(dim, 3 * hw), tp, heads, hd, l == 0)
            o = lax.all_to_all(o, 'tp', 0, 0, tiled=True)
            last = l == n_layers - 1
            nxt = fin if last else mods[l + 1][:2]
            m8 = jnp.concatenate([mods[l], nxt], axis=0)
            res = token_block(o, x, gath[l], kcs[l], vcs[l], m8, w16, b16, last)
            if not last:
                x, a = res
                src = lax.all_gather(a, 'tp', axis=0, tiled=True)
        eps = lax.all_gather(res[:, :4 * keep], ('cfg', 'tp'), axis=0, tiled=True)
        side = x_t.shape[1]
        g = side // 2
        eps = eps.reshape(n_cfg, g, g, 2, 2, keep).transpose(0, 1, 3, 2, 4, 5).reshape(n_cfg, side, side, keep)
        eu = eps[n_cfg // 2:]
        e = eu + GUIDANCE * (eps[:n_cfg // 2] - eu)
        at = alpha_bar[:, 0][:, None, None, None]
        ap = alpha_bar[:, 1][:, None, None, None]
        x0 = (x_t - jnp.sqrt(1.0 - at) * e) / jnp.sqrt(at)
        return jnp.sqrt(ap) * x0 + jnp.sqrt(1.0 - ap) * e

    return jax.shard_map(local_step, mesh=mesh, in_specs=in_specs, out_specs=part_spec, check_vma=False)
```

```python
import functools

import jax
import jax.numpy as jnp
from jax import lax
from jax.experimental import pallas as pl
from jax.experimental.pallas import tpu as pltpu
from jax.sharding import PartitionSpec as P

GUIDANCE = 4.5
LN_EPS = 1e-6
LOG2E = 1.4426950408889634
NT = (((1,), (1,)), ((), ()))
BF = jnp.bfloat16
F32 = jnp.float32
MESH = pl.DeviceIdType.MESH
VMEM_SPEC = pl.BlockSpec(memory_space=pltpu.VMEM)
HBM_SPEC = pl.BlockSpec(memory_space=pl.ANY)
N_KIND = 12
KEY_BLOCK = 512


def layer_norm(values):
    mean_val = jnp.mean(values, axis=-1, keepdims=True)
    centered = values - mean_val
    variance = jnp.mean(centered * centered, axis=-1, keepdims=True)
    return centered * lax.rsqrt(variance + LN_EPS)


def dot(a, b):
    return jnp.dot(a, b, preferred_element_type=F32)


def dot_nt(a, b):
    return lax.dot_general(a, b, NT, preferred_element_type=F32)


class Place:
    def __init__(self, tp, n_cfg):
        self.tp, self.n_cfg = tp, n_cfg
        self.t = lax.axis_index("tp")
        self.y = lax.axis_index("cfg")
        self.right = lax.rem(self.t + 2, tp)
        self.left = lax.rem(self.t + tp - 2, tp)
        self.far = lax.rem(self.t + 4, tp)
        self.mate = mate_of(self.t)
        self.up = lax.rem(self.y + 1, n_cfg)
        self.down = lax.rem(self.y + n_cfg - 1, n_cfg)
        same = (self.t, self.left, self.right, self.far)
        self.slots = same + tuple(mate_of(s) for s in same)

    def barrier(self):
        sem = pltpu.get_barrier_semaphore()
        for r in range(1, self.tp):
            pl.semaphore_signal(sem, inc=1, device_id={"tp": lax.rem(self.t + r, self.tp)}, device_id_type=MESH)
        for r in range(1, self.n_cfg):
            pl.semaphore_signal(sem, inc=1, device_id={"cfg": lax.rem(self.y + r, self.n_cfg)}, device_id_type=MESH)
        pl.semaphore_wait(sem, self.tp + self.n_cfg - 2)


def mate_of(t):
    return t + 1 - 2 * lax.rem(t, 2)


class Gather:
    def __init__(self, place, own, full, sems, sem_base, div):
        self.pc, self.own, self.full, self.sems, self.sem_base, self.div = place, own, full, sems, sem_base, div
        self.unit = own.shape[0] // div
        self.todo = [int(c) for c in {"1": "0125", "2": "01245", "4": "012345"}[str(div)]]
        self.p0 = (self.unit // 2 + 7) // 8 * 8
        self.p1 = self.unit - self.p0
        self.u = lax.rem(place.y, div)

    def copy(self, kind, src, dst, **dev):
        send, recv = self.sems
        return pltpu.make_async_remote_copy(src_ref=src, dst_ref=dst, send_sem=send.at[self.sem_base + kind],
                                            recv_sem=recv.at[self.sem_base + kind], device_id=dev, device_id_type=MESH)

    def part(self, unit, d):
        start = unit * self.unit
        if d is None:
            return pl.ds(pl.multiple_of(start, 8), self.unit)
        return pl.ds(pl.multiple_of(start + d * self.p0, 8), (self.p0, self.p1)[d])

    def x(self, d):
        rows = self.part(self.u, None)
        return self.copy(d, self.own.at[rows], self.full.at[1 + d, rows], tp=(self.pc.right, self.pc.left)[d])

    def f(self, d):
        pc = self.pc
        rows = self.part(self.u, d)
        return self.copy(2 + d, self.full.at[1 + d, rows], self.full.at[3, rows], tp=(pc.right, pc.left)[d])

    def v(self, far, d):
        ref = self.full.at[(pl.ds(1, 2), pl.ds(3, 1))[far], self.part(self.u, d if self.div == 2 else None)]
        return self.copy(4 + 2 * far + d, ref, ref, cfg=(self.pc.up, self.pc.down)[d])

    def w(self, d):
        unit = lax.rem(self.u + (self.div - 1, 1)[d], self.div)
        ref = self.full.at[pl.ds(1, 3), self.part(unit, d)]
        return self.copy(8 + d, ref, ref, cfg=(self.pc.up, self.pc.down)[d])

    def c(self, own):
        if own:
            return self.copy(11, self.own, self.full.at[4], tp=self.pc.mate)
        return self.copy(10, self.full.at[pl.ds(1, 3)], self.full.at[pl.ds(5, 3)], tp=self.pc.mate)

    def run(self, stage):
        ends = range(2)
        vert = ends if self.div > 1 else ()
        if stage == 0:
            for d in ends:
                self.x(d).start()
            self.c(True).start()
        elif stage == 1:
            for d in ends:
                self.x(d).wait_recv()
                self.f(d).start()
            for d in vert:
                self.v(0, d).start()
        elif stage == 2:
            for d in ends:
                self.f(d).wait_recv()
            for d in vert:
                self.v(1, d).start()
            if self.div == 1:
                self.c(False).start()
        elif stage == 3:
            for d in ends:
                self.v(0, d).wait_recv()
                self.v(1, d).wait_recv()
                self.w(d).start()
        elif stage == 4:
            for d in ends:
                if self.div == 4:
                    self.w(d).wait_recv()
                else:
                    self.v(0, d).wait_recv()
                    self.v(1, d).wait_recv()
            self.c(False).start()
        else:
            self.c(True).wait_recv()
            self.c(False).wait_recv()

    def advance(self):
        if self.todo:
            self.run(self.todo.pop(0))

    def require(self):
        while self.todo:
            self.advance()

    def finish(self):
        self.require()
        for d in range(2):
            self.x(d).wait_send()
            self.f(d).wait_send()
            if self.div > 1:
                self.v(0, d).wait_send()
                self.v(1, d).wait_send()
            if self.div == 4:
                self.w(d).wait_send()
        self.c(True).wait_send()
        self.c(False).wait_send()


def chunk_own(name, owns, layer):
    if name == "L":
        return owns[5]
    if name in "ABC":
        return owns["ABC".index(name)].at[layer]
    rows = owns[3].shape[1]
    if name in "DEFG":
        k, n = "DEFG".index(name), rows // 2
    else:
        k, n = "defghijk".index(name), rows // 4
    per = rows // n
    return owns[3 + k // per].at[layer, pl.ds(k % per * n, n)]


def chunk_shape(name, owns, tp):
    if name == "L":
        return jax.ShapeDtypeStruct((tp,) + owns[5].shape, BF)
    rows = owns[0].shape[1] if name in "ABC" else owns[3].shape[1] // (2 if name in "DEFG" else 4)
    return jax.ShapeDtypeStruct((tp, rows, owns[0].shape[2]), BF)


SLOTS = "0123456789abcdefghijklmnopqrstuvwxyzABCDEFGHIJKLMNOP"
PLAN = (("ABLCDEFG", "22124444", "02345679"), ("ABCDEFG", "2224444", "deghikm"))
STEP = 2


def copy_to(src, dst, send_sem, recv_sem, **dev):
    return pltpu.make_async_remote_copy(src_ref=src, dst_ref=dst, send_sem=send_sem, recv_sem=recv_sem, device_id=dev, device_id_type=MESH)


def step_kernel(cfg, *refs):
    (tp, n_cfg, heads, hd, kb) = cfg
    hid_ref, wqkv_ref, cap_ref, wckv_ref, tab_ref, tb_ref, te_ref, fin_ref, wo_ref, bo_ref, xt_ref, al_ref, len_ref = refs[:13]
    owns = refs[13:18]
    out_ref = refs[18]
    pos = 19
    pc = Place(tp, n_cfg)
    n_chunks = sum(len(p[0]) for p in PLAN)
    fulls = refs[pos:pos + n_chunks]
    (mod_ref, wbuf, wa, wcq, xres, a_vm, h_vm, qc_vm, kv_vm, o_in, o_vm, q_vm, k_vm, vt_vm, s0, s1, eps_vm, xt_vm,
     in_sems, w_sems, a_send, a_recv, g_send, g_recv, o_send, o_get, e_send, e_recv, ready) = refs[pos + n_chunks:]
    owns += (kv_vm.at[0],)
    gathers, starts = {}, {}
    for layer, (names, divs, at) in enumerate(PLAN):
        for n, div, slot in zip(names, divs, at):
            i = len(gathers)
            gathers[layer, n] = Gather(pc, chunk_own(n, owns, layer), fulls[i], (g_send, g_recv), i * N_KIND, int(div))
            starts[layer, n] = SLOTS.index(slot)

    def slot_events(slot):
        return [key for key, first in starts.items() if slot >= first and (slot - first) % STEP == 0 and len(gathers[key].todo) > 1]

    def tick(slot):
        for key in slot_events(slot):
            gathers[key].advance()

    def loop_ticks(i, base, count):
        for k in range(count):
            if slot_events(base + k):
                @pl.when(i == k)
                def _():
                    tick(base + k)

    n_tok, dim = hid_ref.shape
    blk = n_tok // tp
    hw = heads * hd
    scale = hd ** -0.5 * LOG2E
    part_rows = wbuf.shape[0] // 3
    part_of = [pl.ds(i * part_rows, part_rows) for i in range(3)]
    x_vm = wbuf.at[pl.ds(part_rows, n_tok)]
    n0_vm, n1_vm = wbuf.at[pl.ds(0, blk)], wbuf.at[pl.ds(blk, blk)]
    half = blk // 2
    halves = [slice(i * half, (i + 1) * half) for i in range(2)]

    def rows_of(i):
        return pl.ds(pl.multiple_of(i * blk, blk), blk)

    def load(i):
        return pltpu.make_async_copy(hid_ref.at[rows_of(i)], x_vm.at[rows_of(i)], in_sems.at[i])

    def load_w(layer):
        return pltpu.make_async_copy(wqkv_ref.at[layer], wcq.at[pl.ds(0, 3 * hw)], w_sems.at[7, tp + 1])

    def x_half(s, part):
        return x_vm.at[pl.ds(pl.multiple_of(s * blk + part * half, half), half)]

    def ax(i):
        d, part = i // 2, i % 2
        return copy_to(a_vm.at[pl.ds(part * half, half)], x_half(pc.t, part), a_send.at[i], a_recv.at[i], tp=(pc.right, pc.left)[d])

    def af(d):
        ref = x_half((pc.left, pc.right)[d], d)
        return copy_to(ref, ref, a_send.at[4 + d], a_recv.at[4 + d], tp=(pc.right, pc.left)[d])

    def ac(i):
        ref = x_vm.at[rows_of(pc.slots[i])]
        return copy_to(ref if i else a_vm, ref, a_send.at[6 + i], a_recv.at[6 + i], tp=pc.mate)

    def qkv_block(layer, i, x):
        rows = rows_of(i)
        qkv = dot_nt(x, wcq[:3 * hw, :])
        q = qkv[:, :hw] * scale
        lane = lax.broadcasted_iota(jnp.int32, q.shape, 1)
        for h in range(heads):
            q_vm[h, rows, :] = jnp.where((lane >= h * hd) & (lane < (h + 1) * hd), q, 0.0).astype(BF)
        k_vm[rows, :] = qkv[:, hw:2 * hw].astype(BF)
        vt = qkv[:, 2 * hw:].T
        for h in range(heads):
            vt_vm[h, :hd, rows] = vt[h * hd:(h + 1) * hd, :].astype(BF)

    def norm(x, layer, i):
        return (layer_norm(x) * (1.0 + mod_ref[layer, i + 1:i + 2, :]) + mod_ref[layer, i:i + 1, :]).astype(BF)

    def norm_block(i):
        return norm(x_vm[rows_of(i), :].astype(F32), 0, 0)

    def pair_step(i, carry):
        loop_ticks(i, 1, tp // 2)
        load(2 * i + 1).wait()
        n1_vm[...] = norm_block(2 * i + 1)
        qkv_block(0, 2 * i, n0_vm[...])

        @pl.when(2 * i + 2 < tp)
        def _():
            load(2 * i + 2).wait()

        n0_vm[...] = norm_block(jnp.minimum(2 * i + 2, tp - 1))
        qkv_block(0, 2 * i + 1, n1_vm[...])
        return carry

    def gathered_step(i, carry):
        b = pc.t
        for k, slot in enumerate("04125637"):
            b = jnp.where(i == k, pc.slots[int(slot)], b)

        def at(k, *acts):
            @pl.when(i == k)
            def _():
                for act in acts:
                    act()

        loop_ticks(i, 21, tp)
        at(0, own_copy().wait)
        at(1, ac(0).wait_recv)
        at(2, ax(0).wait_recv, af(0).start, ax(3).wait_recv, af(1).start, ax(1).wait_recv, ac(1).start)
        at(3, ax(2).wait_recv, ac(2).start)
        at(4, ac(1).wait_recv)
        at(5, ac(2).wait_recv)
        at(6, af(0).wait_recv, af(1).wait_recv, ac(3).start)
        at(7, ac(3).wait_recv)
        qkv_block(1, b, x_vm[rows_of(b), :])
        return carry

    def own_copy():
        return pltpu.make_async_copy(a_vm, x_vm.at[rows_of(pc.t)], in_sems.at[0])

    qb = 2 * blk
    qs = qb // 4
    n_q, n_kb = n_tok // qb, n_tok // kb
    bufs = (s0, s1)

    def o_copy(layer, dest, src):
        return copy_to(o_vm.at[dest], o_in.at[layer, src], o_send.at[layer, dest], o_get.at[layer, src], tp=dest)

    def o_local(layer):
        return pltpu.make_async_copy(o_vm.at[pc.t], o_in.at[layer, pc.t], in_sems.at[0])

    def q_block(k):
        return lax.rem(k + lax.div(pc.t, 2) + 1, n_q)

    def send_o(layer, k):
        for u in range(2):
            dest = q_block(k) * 2 + u

            @pl.when(dest != pc.t)
            def _():
                o_copy(layer, dest, pc.t).start()

            @pl.when(dest == pc.t)
            def _():
                o_local(layer).start()

    def q_step(layer, i, carry):
        h = lax.rem(i, heads)
        k = lax.div(i, heads)
        loop_ticks(i, (5, 29)[layer], heads * n_q)

        @pl.when((h == 0) & (k > 0))
        def _():
            send_o(layer, k - 1)

        qi = q_block(k)
        cols = range(4)

        def scores(j, c):
            q = q_vm[h, pl.ds(pl.multiple_of(qi * qb + c * qs, qs), qs), :]
            s = dot_nt(k_vm[j * kb:(j + 1) * kb, :], q)
            bufs[j % 2][:kb, c * qs:(c + 1) * qs] = s
            return jnp.max(jnp.max(s.reshape(kb // 8, 8, qs), axis=0), axis=0, keepdims=True)

        def weighted(j, c, m):
            pv = None
            for r in range(0, kb, qs):
                p = jnp.exp2(bufs[j % 2][r:r + qs, c * qs:(c + 1) * qs] - m).astype(BF)
                part = dot(vt_vm[h, :, j * kb + r:j * kb + r + qs], p)
                pv = part if pv is None else pv + part
            return pv

        m = [scores(0, c) for c in cols]
        acc = [None for c in cols]
        for j in range(n_kb):
            for c in cols:
                blk_max = scores(j + 1, c) if j + 1 < n_kb else None
                pv = weighted(j, c, m[c])
                acc[c] = pv if j == 0 else acc[c] + pv
                if blk_max is not None:
                    m_new = jnp.maximum(m[c], blk_max)
                    acc[c] = acc[c] * jnp.exp2(m[c] - m_new)
                    m[c] = m_new
        for c in cols:
            o = (acc[c][:hd] / acc[c][hd:hd + 1]).astype(BF)
            o_vm[qi * 2 + c // 2, h, :, (c % 2) * qs:(c % 2 + 1) * qs] = o
        return carry

    def attention(layer):
        lax.fori_loop(0, heads * n_q, functools.partial(q_step, layer), 0)
        send_o(layer, n_q - 1)
        for s in range(tp):
            @pl.when(s != pc.t)
            def _():
                o_copy(layer, s, s).wait_send()
                o_copy(layer, s, s).wait_recv()
        o_local(layer).wait()

    def pull(layer, which, part, dst):
        rows = owns[which].shape[1]
        n = rows // 2
        names = ("ABC"[which],) if which < 3 else ("DEFG"[2 * which - 6 + part],)
        if which > 2 and (layer, names[0]) not in gathers:
            i = 4 * which - 12 + 2 * part
            names = ("defghijk"[i], "defghijk"[i + 1])
        size = gathers[layer, names[0]].full.shape[1]
        res = []
        for k in range(tp):
            for u, name in enumerate(names):
                src = chunk_own(name, owns, layer) if k == 0 else gathers[layer, name].full.at[k]
                start = pc.slots[k] * size * len(names) + u * size
                res.append(pltpu.make_async_copy(src, dst.at[pl.ds(pl.multiple_of(start, 8), size)], w_sems.at[which + 2 * part, len(res)]))
        return [(layer, n) for n in names], res

    def fetch(*args):
        keys, copies = pull(*args)
        for key in keys:
            gathers[key].require()
        for c in copies:
            c.start()

    def ready_w(*args):
        for c in pull(*args)[1]:
            c.wait()

    def kv_copies():
        return [pltpu.make_async_copy(gathers[0, "L"].full.at[k], kv_vm.at[k], w_sems.at[7, k]) for k in range(1, tp)]

    def tokens(layer, base):
        loc = heads
        n_heads = tp * loc

        def mod(i):
            return mod_ref[layer, i:i + 1, :]

        fetch(layer, 0, 0, wa)
        fetch(layer, 1, 0, wcq)
        if layer == 0:
            gathers[0, "L"].require()
            for c in kv_copies():
                c.start()
        tick(base)
        ready_w(layer, 0, 0, wa)
        if layer == 0:
            x_load.wait()
        x1 = []
        for sl in halves:
            o = jnp.concatenate([o_in[layer, s, h, :, sl].astype(F32) for s in range(tp) for h in range(loc)], axis=0).T.astype(BF)
            x0 = a_vm[sl, :].astype(F32) if layer == 0 else xres[sl, :]
            x1.append(x0 + mod(2) * dot(o, wa[...]).astype(BF).astype(F32))
        fetch(layer, 2, 0, wa)
        w1_at, w2_at = (part_of[0], part_of[1]), (part_of[2], part_of[0])
        fetch(layer, 3, 0, wbuf.at[w1_at[0]])
        ready_w(layer, 1, 0, wcq)
        for i, sl in enumerate(halves):
            qt = (dot_nt(x1[i].astype(BF), wcq[...]) * scale).T
            for h in range(n_heads):
                qc_vm[h, :, sl] = qt[h * hd:(h + 1) * hd, :].astype(BF)
        tick(base + 1)
        if layer == 0:
            for c in kv_copies():
                c.wait()
        n_key = kv_vm.shape[1]
        ones = jnp.where(lax.broadcasted_iota(jnp.int32, (80 - hd, n_key), 0) == 0, 1.0, 0.0)
        lane0 = layer * 2 * hw
        key_bias = jnp.where(lax.broadcasted_iota(jnp.int32, (n_key, blk), 0) < jnp.minimum(len_ref[0], cap_ref.shape[0]), 0.0, -1e30)

        def cross_scores(n):
            k, h = n // loc, n % loc
            return dot(kv_vm[k, :, lane0 + h * hd:lane0 + (h + 1) * hd], qc_vm[pc.slots[k] * loc + h]) + key_bias

        s_next = cross_scores(0)
        for n in range(n_heads):
            k, h = n // loc, n % loc
            if n == tp:
                tick(base + 2)
            if h == 0:
                v_t = kv_vm[k, :, lane0 + hw:lane0 + 2 * hw].astype(F32).T
            s = s_next
            if n + 1 < n_heads:
                s_next = cross_scores(n + 1)
            p = jnp.exp2(s - jnp.max(s, axis=0, keepdims=True)).astype(BF)
            vt = jnp.concatenate([v_t[h * hd:(h + 1) * hd], ones], axis=0).astype(BF)
            pv = dot(vt, p)
            s0[pl.ds(pl.multiple_of((pc.slots[k] * loc + h) * hd, 8), hd), :blk] = (pv[:hd] / pv[hd:hd + 1]).astype(BF).astype(F32)
        tick(base + 3)
        fetch(layer, 3, 1, wbuf.at[w1_at[1]])
        ready_w(layer, 2, 0, wa)
        x2, a2 = [], []
        for i, sl in enumerate(halves):
            oc = s0[:, sl].T.astype(BF)
            x2.append(x1[i] + dot(oc, wa[...]).astype(BF).astype(F32))
            a2.append(norm(x2[i], layer, 3))
        tick(base + 4)
        fetch(layer, 4, 0, wbuf.at[w2_at[0]])
        step = part_rows // 2
        order = [(j, i) for j in range(4) for i in range(2)]

        def fc1(j, i):
            return dot_nt(a2[i], wbuf[j * step:(j + 1) * step, :])

        ready_w(layer, 3, 0, wbuf.at[w1_at[0]])
        h_next = fc1(*order[0])
        for n, (j, i) in enumerate(order):
            if (j, i) == (1, 1):
                tick(base + 5)
                ready_w(layer, 3, 1, wbuf.at[w1_at[1]])
            hidden = h_next
            if n + 1 < len(order):
                h_next = fc1(*order[n + 1])
            h_vm[halves[i], j * step:(j + 1) * step] = jax.nn.gelu(hidden, approximate=True).astype(BF)
        tick(base + 6)
        fetch(layer, 4, 1, wbuf.at[w2_at[1]])
        ready_w(layer, 4, 0, wbuf.at[w2_at[0]])
        y = [dot(h_vm[sl, :part_rows], wbuf[w2_at[0], :]) for sl in halves]
        if layer == 0:
            for i, dev in enumerate((pc.left, pc.right, pc.mate)):
                pl.semaphore_signal(ready.at[i], inc=1, device_id={"tp": dev}, device_id_type=MESH)
        tick(base + 7)
        ready_w(layer, 4, 1, wbuf.at[w2_at[1]])
        res = []
        for i, sl in enumerate(halves):
            x3 = x2[i] + mod(5) * (y[i] + dot(h_vm[sl, part_rows:], wbuf[w2_at[1], :])).astype(BF).astype(F32)
            if layer == 0:
                xres[sl, :] = x3
                a_vm[sl, :] = norm(x3, layer, 6)
            else:
                res.append(dot_nt(wo_ref[...], norm(x3, layer, 6)))
        return res

    for i in range(tp):
        load(i).start()
    x_load = pltpu.make_async_copy(hid_ref.at[rows_of(pc.t)], a_vm, w_sems.at[7, tp])
    x_load.start()
    row_id = lax.broadcasted_iota(jnp.int32, (80 - hd, n_tok), 0)
    for h in range(heads):
        vt_vm[h, hd:, :] = jnp.where(row_id == 0, 1.0, 0.0).astype(BF)
    n_cap = cap_ref.shape[0]
    wckv_vm = wa.at[pl.ds(0, wckv_ref.shape[0])]
    n_rows = eps_vm.shape[1]
    mine = pl.ds(pc.t * n_rows, n_rows)
    loads = [load_w(0), pltpu.make_async_copy(xt_ref.at[:, mine], xt_vm, w_sems.at[1, tp]), pltpu.make_async_copy(wckv_ref, wckv_vm, w_sems.at[0, tp])]
    for c in loads:
        c.start()
    row = lax.rem(pc.y, tb_ref.shape[0])
    n_layers = tab_ref.shape[0]
    for l in range(n_layers):
        mod_ref[l, :6, :] = tab_ref[l].astype(F32) + tb_ref[row].astype(F32)
    for l in range(n_layers):
        mod_ref[l, 6:, :] = fin_ref[...].astype(F32) + te_ref[row].astype(F32) if l == n_layers - 1 else mod_ref[l + 1, :2, :]
    pc.barrier()
    tick(0)
    for c in loads:
        c.wait()
    kv_vm[0, n_cap:, :] = jnp.zeros((kv_vm.shape[1] - n_cap, kv_vm.shape[2]), BF)
    kv_vm[0, :n_cap, :] = dot_nt(cap_ref[...], wckv_vm[...]).astype(BF)
    load(0).wait()
    n0_vm[...] = norm_block(0)
    lax.fori_loop(0, tp // 2, pair_step, 0)
    attention(0)
    tokens(0, 13)
    load_w(1).start()
    own_copy().start()
    for i in range(3):
        pl.semaphore_wait(ready.at[i], 1)
    for i in "0312":
        ax(int(i)).start()
    ac(0).start()
    load_w(1).wait()
    lax.fori_loop(0, tp, gathered_step, 0)
    attention(1)
    for i in range(4):
        ax(i).wait_send()
        ac(i).wait_send()
    for d in range(2):
        af(d).wait_send()
    e = jnp.concatenate(tokens(1, 37), axis=1) + bo_ref[...].astype(F32).T
    n_rows, n_ch, width = eps_vm.shape[1:]
    n_pairs = n_rows // 2
    src = lax.broadcasted_iota(jnp.int32, (blk, n_pairs * width), 0)
    dst = lax.broadcasted_iota(jnp.int32, (blk, n_pairs * width), 1)
    spread = jnp.where(src == lax.shift_right_logical(dst, 1), 1.0, 0.0).astype(BF)
    hi = e.astype(BF)
    r1 = e - hi.astype(F32)
    mid = r1.astype(BF)
    lo = (r1 - mid.astype(F32)).astype(BF)
    wide = dot(hi, spread) + dot(mid, spread) + dot(lo, spread)
    odd = lax.rem(lax.broadcasted_iota(jnp.int32, (n_ch, width), 1), 2) == 1
    for i in range(n_pairs):
        for p in range(2):
            lanes = slice(i * width, (i + 1) * width)
            q0 = wide[4 * p * n_ch:(4 * p + 1) * n_ch, lanes]
            q1 = wide[(4 * p + 2) * n_ch:(4 * p + 3) * n_ch, lanes]
            eps_vm[pc.y, 2 * i + p] = jnp.where(odd, q1, q0)

    def e_copy(r):
        return copy_to(eps_vm.at[pc.y], eps_vm.at[pc.y], e_send.at[r], e_recv.at[r], cfg=lax.rem(pc.y + r, n_cfg))

    for r in range(1, n_cfg):
        e_copy(r).start()
    for r in range(1, n_cfg):
        e_copy(r).wait_recv()
    n_img = n_cfg // 2
    for b in range(n_img):
        ec, eu = eps_vm[b], eps_vm[n_img + b]
        guided = eu + GUIDANCE * (ec - eu)
        abar_t, abar_prev = al_ref[b:b + 1, :1], al_ref[b:b + 1, 1:]
        x0 = (xt_vm[b] - jnp.sqrt(1.0 - abar_t) * guided) / jnp.sqrt(abar_t)
        out_ref[b, mine] = jnp.sqrt(abar_prev) * x0 + jnp.sqrt(1.0 - abar_prev) * guided

    def r_copy(r):
        ref = out_ref.at[:, mine]
        return copy_to(ref, ref, e_send.at[n_cfg + r], e_recv.at[n_cfg + r], tp=lax.rem(pc.t + r, tp))

    for r in range(1, tp):
        r_copy(r).start()
    for r in range(1, tp):
        r_copy(r).wait_recv()
    for r in range(1, n_cfg):
        e_copy(r).wait_send()
    for r in range(1, tp):
        r_copy(r).wait_send()
    for key in gathers:
        gathers[key].finish()


def sampling_step(args, owns, tp, n_cfg, heads, hd):
    n_tok, dim = args[0].shape
    xt = args[10]
    blk, hw, kb = n_tok // tp, heads * hd, KEY_BLOCK
    dma = pltpu.SemaphoreType.DMA
    n_chunks = sum(len(p[0]) for p in PLAN)
    n_layers = args[1].shape[0]
    kv = jax.ShapeDtypeStruct((-(-args[2].shape[0] // 16) * 16, args[3].shape[0]), BF)
    n_ff = tp * owns[3].shape[1]
    o_shape = (tp, heads, hd, blk)
    vmem = [
        ((n_layers, 8, dim), F32), ((3 * n_ff // 2, dim), BF), ((tp * hw, dim), BF), ((tp * hw, dim), BF), ((blk, dim), F32), ((blk, dim), BF), ((blk, n_ff), BF),
        ((tp * heads, hd, blk), BF), ((tp,) + kv.shape, BF), ((n_layers,) + o_shape, BF), (o_shape, BF),
        ((heads, n_tok, hw), BF), ((n_tok, hw), BF), ((heads, 80, n_tok), BF), ((max(kb, tp * hw), 2 * blk), F32), ((kb, 2 * blk), F32),
        ((n_cfg, xt.shape[1] // tp) + xt.shape[2:], F32), ((xt.shape[0], xt.shape[1] // tp) + xt.shape[2:], F32),
    ]
    res = pl.pallas_call(
        functools.partial(step_kernel, (tp, n_cfg, heads, hd, kb)),
        out_shape=[jax.ShapeDtypeStruct(xt.shape, F32)] + [chunk_shape(n, owns + (kv,), tp) for p in PLAN for n in p[0]],
        in_specs=[HBM_SPEC] * 2 + [VMEM_SPEC, HBM_SPEC] + [VMEM_SPEC] * 6 + [HBM_SPEC, VMEM_SPEC, pl.BlockSpec(memory_space=pltpu.SMEM)] + [HBM_SPEC] * 5,
        out_specs=[VMEM_SPEC] + [HBM_SPEC] * n_chunks,
        scratch_shapes=[pltpu.VMEM(*v) for v in vmem] + [
            dma((tp,)), dma((8, 2 * tp)), dma((10,)), dma((10,)), dma((n_chunks * N_KIND,)), dma((n_chunks * N_KIND,)),
            dma((n_layers, tp)), dma((n_layers, tp)), dma((n_cfg + tp,)), dma((n_cfg + tp,)), pltpu.SemaphoreType.REGULAR((3,)),
        ],
        compiler_params=pltpu.CompilerParams(vmem_limit_bytes=67043328, collective_id=1, has_side_effects=True),
    )(*args, *owns)
    return res[0]


def solution(mesh):
    row_spec = P(('dp', 'cfg'))
    part_spec = P('dp')
    def tp_at(k):
        return P(*[None] * k, 'tp')

    in_specs = (row_spec,) * 3 + (part_spec,) * 4 + (P(), tp_at(3), tp_at(1), tp_at(2), tp_at(3), tp_at(1), tp_at(2), tp_at(1)) + (P(),) * 3
    tp = mesh.shape['tp']
    n_cfg = mesh.shape['cfg']

    def local_step(hidden, caption, cap_len, t_block, t_embed, x_t, alpha_bar, mod_table, w_qkv, w_proj, w_cq, w_ckv, w_cproj, w_fc1, w_fc2, final_table, w_out, b_out):
        dim = hidden.shape[2]
        n_layers, _, _, heads, hd = w_qkv.shape

        def rows_major(w, lead):
            return jnp.moveaxis(w, 1, -1).reshape(*lead, -1, dim)

        owns = (w_proj.reshape(n_layers, -1, dim), rows_major(w_cq, (n_layers,)), w_cproj.reshape(n_layers, -1, dim), w_fc1.mT, w_fc2)
        args = (hidden[0], rows_major(w_qkv, (n_layers,)), caption[0], rows_major(w_ckv, ()), mod_table, t_block.reshape(t_block.shape[0], -1, dim),
                t_embed[:, None], final_table, w_out.mT, b_out[None], x_t.mT, alpha_bar, cap_len)
        return sampling_step(args, owns, tp, n_cfg, heads, hd).mT

    return jax.shard_map(local_step, mesh=mesh, in_specs=in_specs, out_specs=part_spec, check_vma=False)
```

```python
import functools

import jax
import jax.numpy as jnp
from jax import lax
from jax.experimental import pallas as pl
from jax.experimental.pallas import tpu as pltpu
from jax.sharding import PartitionSpec as P

GUIDANCE = 4.5
LN_EPS = 1e-6
LOG2E = 1.4426950408889634
NT = (((1,), (1,)), ((), ()))
BF = jnp.bfloat16
F32 = jnp.float32
MESH = pl.DeviceIdType.MESH
VMEM_SPEC = pl.BlockSpec(memory_space=pltpu.VMEM)
HBM_SPEC = pl.BlockSpec(memory_space=pl.ANY)
N_KIND = 12
KEY_BLOCK = 512


def layer_norm(values):
    mean_val = jnp.mean(values, axis=-1, keepdims=True)
    centered = values - mean_val
    variance = jnp.mean(centered * centered, axis=-1, keepdims=True)
    return centered * lax.rsqrt(variance + LN_EPS)


def dot(a, b):
    return jnp.dot(a, b, preferred_element_type=F32)


def dot_nt(a, b):
    return lax.dot_general(a, b, NT, preferred_element_type=F32)


class Place:
    def __init__(self, tp, n_cfg):
        self.tp, self.n_cfg = tp, n_cfg
        self.t = lax.axis_index("tp")
        self.y = lax.axis_index("cfg")
        self.right = lax.rem(self.t + 2, tp)
        self.left = lax.rem(self.t + tp - 2, tp)
        self.far = lax.rem(self.t + 4, tp)
        self.mate = mate_of(self.t)
        self.up = lax.rem(self.y + 1, n_cfg)
        self.down = lax.rem(self.y + n_cfg - 1, n_cfg)
        same = (self.t, self.left, self.right, self.far)
        self.slots = same + tuple(mate_of(s) for s in same)

    def barrier(self):
        sem = pltpu.get_barrier_semaphore()
        for r in range(1, self.tp):
            pl.semaphore_signal(sem, inc=1, device_id={"tp": lax.rem(self.t + r, self.tp)}, device_id_type=MESH)
        for r in range(1, self.n_cfg):
            pl.semaphore_signal(sem, inc=1, device_id={"cfg": lax.rem(self.y + r, self.n_cfg)}, device_id_type=MESH)
        pl.semaphore_wait(sem, self.tp + self.n_cfg - 2)


def mate_of(t):
    return t + 1 - 2 * lax.rem(t, 2)


class Gather:
    def __init__(self, place, own, full, sems, sem_base, div):
        self.pc, self.own, self.full, self.sems, self.sem_base, self.div = place, own, full, sems, sem_base, div
        self.unit = own.shape[0] // div
        self.todo = [int(c) for c in {"1": "0125", "2": "01245", "4": "012345"}[str(div)]]
        self.p0 = (self.unit // 2 + 7) // 8 * 8
        self.p1 = self.unit - self.p0
        self.u = lax.rem(place.y, div)

    def copy(self, kind, src, dst, **dev):
        send, recv = self.sems
        return pltpu.make_async_remote_copy(src_ref=src, dst_ref=dst, send_sem=send.at[self.sem_base + kind],
                                            recv_sem=recv.at[self.sem_base + kind], device_id=dev, device_id_type=MESH)

    def part(self, unit, d):
        start = unit * self.unit
        if d is None:
            return pl.ds(pl.multiple_of(start, 8), self.unit)
        return pl.ds(pl.multiple_of(start + d * self.p0, 8), (self.p0, self.p1)[d])

    def x(self, d):
        rows = self.part(self.u, None)
        return self.copy(d, self.own.at[rows], self.full.at[1 + d, rows], tp=(self.pc.right, self.pc.left)[d])

    def f(self, d):
        pc = self.pc
        rows = self.part(self.u, d)
        return self.copy(2 + d, self.full.at[1 + d, rows], self.full.at[3, rows], tp=(pc.right, pc.left)[d])

    def v(self, far, d):
        ref = self.full.at[(pl.ds(1, 2), pl.ds(3, 1))[far], self.part(self.u, d if self.div == 2 else None)]
        return self.copy(4 + 2 * far + d, ref, ref, cfg=(self.pc.up, self.pc.down)[d])

    def w(self, d):
        unit = lax.rem(self.u + (self.div - 1, 1)[d], self.div)
        ref = self.full.at[pl.ds(1, 3), self.part(unit, d)]
        return self.copy(8 + d, ref, ref, cfg=(self.pc.up, self.pc.down)[d])

    def c(self, own):
        if own:
            return self.copy(11, self.own, self.full.at[4], tp=self.pc.mate)
        return self.copy(10, self.full.at[pl.ds(1, 3)], self.full.at[pl.ds(5, 3)], tp=self.pc.mate)

    def run(self, stage):
        ends = range(2)
        vert = ends if self.div > 1 else ()
        if stage == 0:
            for d in ends:
                self.x(d).start()
            self.c(True).start()
        elif stage == 1:
            for d in ends:
                self.x(d).wait_recv()
                self.f(d).start()
            for d in vert:
                self.v(0, d).start()
        elif stage == 2:
            for d in ends:
                self.f(d).wait_recv()
            for d in vert:
                self.v(1, d).start()
            if self.div == 1:
                self.c(False).start()
        elif stage == 3:
            for d in ends:
                self.v(0, d).wait_recv()
                self.v(1, d).wait_recv()
                self.w(d).start()
        elif stage == 4:
            for d in ends:
                if self.div == 4:
                    self.w(d).wait_recv()
                else:
                    self.v(0, d).wait_recv()
                    self.v(1, d).wait_recv()
            self.c(False).start()
        else:
            self.c(True).wait_recv()
            self.c(False).wait_recv()

    def advance(self):
        if self.todo:
            self.run(self.todo.pop(0))

    def require(self):
        while self.todo:
            self.advance()

    def finish(self):
        self.require()
        for d in range(2):
            self.x(d).wait_send()
            self.f(d).wait_send()
            if self.div > 1:
                self.v(0, d).wait_send()
                self.v(1, d).wait_send()
            if self.div == 4:
                self.w(d).wait_send()
        self.c(True).wait_send()
        self.c(False).wait_send()


def chunk_own(name, owns, layer):
    if name == "L":
        return owns[5]
    if name in "ABC":
        return owns["ABC".index(name)].at[layer]
    rows = owns[3].shape[1]
    if name in "DEFG":
        k, n = "DEFG".index(name), rows // 2
    else:
        k, n = "defghijk".index(name), rows // 4
    per = rows // n
    return owns[3 + k // per].at[layer, pl.ds(k % per * n, n)]


def chunk_shape(name, owns, tp):
    if name == "L":
        return jax.ShapeDtypeStruct((tp,) + owns[5].shape, BF)
    rows = owns[0].shape[1] if name in "ABC" else owns[3].shape[1] // (2 if name in "DEFG" else 4)
    return jax.ShapeDtypeStruct((tp, rows, owns[0].shape[2]), BF)


SLOTS = "0123456789abcdefghijklmnopqrstuvwxyzABCDEFGHIJKLMNOP"
PLAN = (
    ("B21356", "D401246", "C2145a", "G2cfhi", "F417bcd", "A247ab", "L159c", "E416adg"),
    ("D4ejopu", "B2ckny", "G44kmnr", "E2wBCE", "C28iwy", "F4jstvC", "A2hijn"),
)


def copy_to(src, dst, send_sem, recv_sem, **dev):
    return pltpu.make_async_remote_copy(src_ref=src, dst_ref=dst, send_sem=send_sem, recv_sem=recv_sem, device_id=dev, device_id_type=MESH)


def step_kernel(cfg, *refs):
    (tp, n_cfg, heads, hd, kb) = cfg
    hid_ref, wqkv_ref, cap_ref, wckv_ref, tab_ref, tb_ref, te_ref, fin_ref, wo_ref, bo_ref, xt_ref, al_ref, len_ref = refs[:13]
    owns = refs[13:18]
    out_ref = refs[18]
    pos = 19
    pc = Place(tp, n_cfg)
    n_chunks = sum(len(p) for p in PLAN)
    fulls = refs[pos:pos + n_chunks]
    (mod_ref, wbuf, wa, wcq, xres, a_vm, h_vm, qc_vm, kv_vm, o_in, o_vm, q_vm, k_vm, vt_vm, s0, s1, eps_vm, xt_vm,
     in_sems, w_sems, a_send, a_recv, g_send, g_recv, o_send, o_get, e_send, e_recv, ready) = refs[pos + n_chunks:]
    owns += (kv_vm.at[0],)
    gathers, starts = {}, {}
    for layer, chunks in enumerate(PLAN):
        for entry in chunks:
            i = len(gathers)
            gathers[layer, entry[0]] = Gather(pc, chunk_own(entry[0], owns, layer), fulls[i], (g_send, g_recv), i * N_KIND, int(entry[1]))
            starts[layer, entry[0]] = [SLOTS.index(c) for c in entry[2:]]

    def slot_events(slot):
        return [key for key, at in starts.items() if slot in at and len(gathers[key].todo) > 1]

    def tick(slot):
        for key in slot_events(slot):
            gathers[key].advance()

    def loop_ticks(i, base, count):
        for k in range(count):
            if slot_events(base + k):
                @pl.when(i == k)
                def _():
                    tick(base + k)

    n_tok, dim = hid_ref.shape
    blk = n_tok // tp
    hw = heads * hd
    scale = hd ** -0.5 * LOG2E
    part_rows = wbuf.shape[0] // 3
    part_of = [pl.ds(i * part_rows, part_rows) for i in range(3)]
    x_vm = wbuf.at[pl.ds(part_rows, n_tok)]
    n0_vm, n1_vm = wbuf.at[pl.ds(0, blk)], wbuf.at[pl.ds(blk, blk)]
    half = blk // 2
    halves = [slice(i * half, (i + 1) * half) for i in range(2)]

    def rows_of(i):
        return pl.ds(pl.multiple_of(i * blk, blk), blk)

    def load(i):
        return pltpu.make_async_copy(hid_ref.at[rows_of(i)], x_vm.at[rows_of(i)], in_sems.at[i])

    def load_w(layer):
        return pltpu.make_async_copy(wqkv_ref.at[layer], wcq.at[pl.ds(0, 3 * hw)], w_sems.at[7, tp + 1])

    def x_half(s, part):
        return x_vm.at[pl.ds(pl.multiple_of(s * blk + part * half, half), half)]

    def ax(i):
        d, part = i // 2, i % 2
        return copy_to(a_vm.at[pl.ds(part * half, half)], x_half(pc.t, part), a_send.at[i], a_recv.at[i], tp=(pc.right, pc.left)[d])

    def af(d):
        ref = x_half((pc.left, pc.right)[d], d)
        return copy_to(ref, ref, a_send.at[4 + d], a_recv.at[4 + d], tp=(pc.right, pc.left)[d])

    def ac(i):
        ref = x_vm.at[rows_of(pc.slots[i])]
        return copy_to(ref if i else a_vm, ref, a_send.at[6 + i], a_recv.at[6 + i], tp=pc.mate)

    def qkv_block(layer, i, x):
        rows = rows_of(i)
        qkv = dot_nt(x, wcq[:3 * hw, :])
        q = qkv[:, :hw] * scale
        lane = lax.broadcasted_iota(jnp.int32, q.shape, 1)
        for h in range(heads):
            q_vm[h, rows, :] = jnp.where((lane >= h * hd) & (lane < (h + 1) * hd), q, 0.0).astype(BF)
        k_vm[rows, :] = qkv[:, hw:2 * hw].astype(BF)
        vt = qkv[:, 2 * hw:].T
        for h in range(heads):
            vt_vm[h, :hd, rows] = vt[h * hd:(h + 1) * hd, :].astype(BF)

    def norm(x, layer, i):
        return (layer_norm(x) * (1.0 + mod_ref[layer, i + 1:i + 2, :]) + mod_ref[layer, i:i + 1, :]).astype(BF)

    def norm_block(i):
        return norm(x_vm[rows_of(i), :].astype(F32), 0, 0)

    def pair_step(i, carry):
        loop_ticks(i, 1, tp // 2)
        load(2 * i + 1).wait()
        n1_vm[...] = norm_block(2 * i + 1)
        qkv_block(0, 2 * i, n0_vm[...])

        @pl.when(2 * i + 2 < tp)
        def _():
            load(2 * i + 2).wait()

        n0_vm[...] = norm_block(jnp.minimum(2 * i + 2, tp - 1))
        qkv_block(0, 2 * i + 1, n1_vm[...])
        return carry

    def gathered_step(i, carry):
        b = pc.t
        for k, slot in enumerate("04125637"):
            b = jnp.where(i == k, pc.slots[int(slot)], b)

        def at(k, *acts):
            @pl.when(i == k)
            def _():
                for act in acts:
                    act()

        loop_ticks(i, 21, tp)
        at(0, own_copy().wait)
        at(1, ac(0).wait_recv)
        at(2, ax(0).wait_recv, af(0).start, ax(3).wait_recv, af(1).start, ax(1).wait_recv, ac(1).start)
        at(3, ax(2).wait_recv, ac(2).start)
        at(4, ac(1).wait_recv)
        at(5, ac(2).wait_recv)
        at(6, af(0).wait_recv, af(1).wait_recv, ac(3).start)
        at(7, ac(3).wait_recv)
        qkv_block(1, b, x_vm[rows_of(b), :])
        return carry

    def own_copy():
        return pltpu.make_async_copy(a_vm, x_vm.at[rows_of(pc.t)], in_sems.at[0])

    qb = 2 * blk
    qs = qb // 4
    n_q, n_kb = n_tok // qb, n_tok // kb
    bufs = (s0, s1)

    def o_copy(layer, dest, src):
        return copy_to(o_vm.at[dest], o_in.at[layer, src], o_send.at[layer, dest], o_get.at[layer, src], tp=dest)

    def o_local(layer):
        return pltpu.make_async_copy(o_vm.at[pc.t], o_in.at[layer, pc.t], in_sems.at[0])

    def q_block(k):
        return lax.rem(k + lax.div(pc.t, 2) + 1, n_q)

    def send_o(layer, k):
        for u in range(2):
            dest = q_block(k) * 2 + u

            @pl.when(dest != pc.t)
            def _():
                o_copy(layer, dest, pc.t).start()

            @pl.when(dest == pc.t)
            def _():
                o_local(layer).start()

    def q_step(layer, i, carry):
        h = lax.rem(i, heads)
        k = lax.div(i, heads)
        loop_ticks(i, (5, 29)[layer], heads * n_q)

        @pl.when((h == 0) & (k > 0))
        def _():
            send_o(layer, k - 1)

        qi = q_block(k)
        cols = range(4)

        def scores(j, c):
            q = q_vm[h, pl.ds(pl.multiple_of(qi * qb + c * qs, qs), qs), :]
            s = dot_nt(k_vm[j * kb:(j + 1) * kb, :], q)
            bufs[j % 2][:kb, c * qs:(c + 1) * qs] = s
            return jnp.max(jnp.max(s.reshape(kb // 8, 8, qs), axis=0), axis=0, keepdims=True)

        def weighted(j, c, m):
            pv = None
            for r in range(0, kb, qs):
                p = jnp.exp2(bufs[j % 2][r:r + qs, c * qs:(c + 1) * qs] - m).astype(BF)
                part = dot(vt_vm[h, :, j * kb + r:j * kb + r + qs], p)
                pv = part if pv is None else pv + part
            return pv

        m = [scores(0, c) for c in cols]
        acc = [None for c in cols]
        for j in range(n_kb):
            for c in cols:
                blk_max = scores(j + 1, c) if j + 1 < n_kb else None
                pv = weighted(j, c, m[c])
                acc[c] = pv if j == 0 else acc[c] + pv
                if blk_max is not None:
                    m_new = jnp.maximum(m[c], blk_max)
                    acc[c] = acc[c] * jnp.exp2(m[c] - m_new)
                    m[c] = m_new
        for c in cols:
            o = (acc[c][:hd] / acc[c][hd:hd + 1]).astype(BF)
            o_vm[qi * 2 + c // 2, h, :, (c % 2) * qs:(c % 2 + 1) * qs] = o
        return carry

    def attention(layer):
        lax.fori_loop(0, heads * n_q, functools.partial(q_step, layer), 0)
        send_o(layer, n_q - 1)
        for s in range(tp):
            @pl.when(s != pc.t)
            def _():
                o_copy(layer, s, s).wait_send()
                o_copy(layer, s, s).wait_recv()
        o_local(layer).wait()

    def pull(layer, which, part, dst):
        rows = owns[which].shape[1]
        n = rows // 2
        names = ("ABC"[which],) if which < 3 else ("DEFG"[2 * which - 6 + part],)
        if which > 2 and (layer, names[0]) not in gathers:
            i = 4 * which - 12 + 2 * part
            names = ("defghijk"[i], "defghijk"[i + 1])
        size = gathers[layer, names[0]].full.shape[1]
        res = []
        for k in range(tp):
            for u, name in enumerate(names):
                src = chunk_own(name, owns, layer) if k == 0 else gathers[layer, name].full.at[k]
                start = pc.slots[k] * size * len(names) + u * size
                res.append(pltpu.make_async_copy(src, dst.at[pl.ds(pl.multiple_of(start, 8), size)], w_sems.at[which + 2 * part, len(res)]))
        return [(layer, n) for n in names], res

    def fetch(*args):
        keys, copies = pull(*args)
        for key in keys:
            gathers[key].require()
        for c in copies:
            c.start()

    def ready_w(*args):
        for c in pull(*args)[1]:
            c.wait()

    def kv_copies():
        return [pltpu.make_async_copy(gathers[0, "L"].full.at[k], kv_vm.at[k], w_sems.at[7, k]) for k in range(1, tp)]

    def tokens(layer, base):
        loc = heads
        n_heads = tp * loc

        def mod(i):
            return mod_ref[layer, i:i + 1, :]

        fetch(layer, 0, 0, wa)
        fetch(layer, 1, 0, wcq)
        if layer == 0:
            gathers[0, "L"].require()
            for c in kv_copies():
                c.start()
        tick(base)
        ready_w(layer, 0, 0, wa)
        if layer == 0:
            x_load.wait()
        x1 = []
        for sl in halves:
            o = jnp.concatenate([o_in[layer, s, h, :, sl].astype(F32) for s in range(tp) for h in range(loc)], axis=0).T.astype(BF)
            x0 = a_vm[sl, :].astype(F32) if layer == 0 else xres[sl, :]
            x1.append(x0 + mod(2) * dot(o, wa[...]).astype(BF).astype(F32))
        fetch(layer, 2, 0, wa)
        w1_at, w2_at = (part_of[0], part_of[1]), (part_of[2], part_of[0])
        ready_w(layer, 1, 0, wcq)
        for i, sl in enumerate(halves):
            qt = (dot_nt(x1[i].astype(BF), wcq[...]) * scale).T
            for h in range(n_heads):
                qc_vm[h, :, sl] = qt[h * hd:(h + 1) * hd, :].astype(BF)
        tick(base + 1)
        if layer == 0:
            for c in kv_copies():
                c.wait()
        n_key = kv_vm.shape[1]
        ones = jnp.where(lax.broadcasted_iota(jnp.int32, (80 - hd, n_key), 0) == 0, 1.0, 0.0)
        lane0 = layer * 2 * hw
        key_bias = jnp.where(lax.broadcasted_iota(jnp.int32, (n_key, blk), 0) < jnp.minimum(len_ref[0], cap_ref.shape[0]), 0.0, -1e30)

        def cross_scores(n):
            k, h = n // loc, n % loc
            return dot(kv_vm[k, :, lane0 + h * hd:lane0 + (h + 1) * hd], qc_vm[pc.slots[k] * loc + h]) + key_bias

        s_next = cross_scores(0)
        for n in range(n_heads):
            k, h = n // loc, n % loc
            if n == tp:
                tick(base + 2)
            if h == 0:
                v_t = kv_vm[k, :, lane0 + hw:lane0 + 2 * hw].astype(F32).T
            s = s_next
            if n + 1 < n_heads:
                s_next = cross_scores(n + 1)
            p = jnp.exp2(s - jnp.max(s, axis=0, keepdims=True)).astype(BF)
            vt = jnp.concatenate([v_t[h * hd:(h + 1) * hd], ones], axis=0).astype(BF)
            pv = dot(vt, p)
            s0[pl.ds(pl.multiple_of((pc.slots[k] * loc + h) * hd, 8), hd), :blk] = (pv[:hd] / pv[hd:hd + 1]).astype(BF).astype(F32)
        tick(base + 3)
        fetch(layer, 3, 0, wbuf.at[w1_at[0]])
        ready_w(layer, 2, 0, wa)
        x2, a2 = [], []
        for i, sl in enumerate(halves):
            oc = s0[:, sl].T.astype(BF)
            x2.append(x1[i] + dot(oc, wa[...]).astype(BF).astype(F32))
            a2.append(norm(x2[i], layer, 3))
        tick(base + 4)
        fetch(layer, 4, 0, wbuf.at[w2_at[0]])
        step = part_rows // 2
        order = [(j, i) for j in range(4) for i in range(2)]

        def fc1(j, i):
            return dot_nt(a2[i], wbuf[j * step:(j + 1) * step, :])

        ready_w(layer, 3, 0, wbuf.at[w1_at[0]])
        h_next = fc1(*order[0])
        for n, (j, i) in enumerate(order):
            if (j, i) == (1, 0):
                fetch(layer, 3, 1, wbuf.at[w1_at[1]])
            if (j, i) == (1, 1):
                tick(base + 5)
                ready_w(layer, 3, 1, wbuf.at[w1_at[1]])
            hidden = h_next
            if n + 1 < len(order):
                h_next = fc1(*order[n + 1])
            h_vm[halves[i], j * step:(j + 1) * step] = jax.nn.gelu(hidden, approximate=True).astype(BF)
        tick(base + 6)
        fetch(layer, 4, 1, wbuf.at[w2_at[1]])
        ready_w(layer, 4, 0, wbuf.at[w2_at[0]])
        y = [dot(h_vm[sl, :part_rows], wbuf[w2_at[0], :]) for sl in halves]
        if layer == 0:
            for i, dev in enumerate((pc.left, pc.right, pc.mate)):
                pl.semaphore_signal(ready.at[i], inc=1, device_id={"tp": dev}, device_id_type=MESH)
        tick(base + 7)
        ready_w(layer, 4, 1, wbuf.at[w2_at[1]])
        res = []
        for i, sl in enumerate(halves):
            x3 = x2[i] + mod(5) * (y[i] + dot(h_vm[sl, part_rows:], wbuf[w2_at[1], :])).astype(BF).astype(F32)
            if layer == 0:
                xres[sl, :] = x3
                a_vm[sl, :] = norm(x3, layer, 6)
            else:
                res.append(dot_nt(wo_ref[...], norm(x3, layer, 6)))
        return res

    for i in range(tp):
        load(i).start()
    x_load = pltpu.make_async_copy(hid_ref.at[rows_of(pc.t)], a_vm, w_sems.at[7, tp])
    x_load.start()
    row_id = lax.broadcasted_iota(jnp.int32, (80 - hd, n_tok), 0)
    for h in range(heads):
        vt_vm[h, hd:, :] = jnp.where(row_id == 0, 1.0, 0.0).astype(BF)
    n_cap = cap_ref.shape[0]
    wckv_vm = wa.at[pl.ds(0, wckv_ref.shape[0])]
    n_rows = eps_vm.shape[1]
    mine = pl.ds(pc.t * n_rows, n_rows)
    loads = [load_w(0), pltpu.make_async_copy(xt_ref.at[:, mine], xt_vm, w_sems.at[1, tp]), pltpu.make_async_copy(wckv_ref, wckv_vm, w_sems.at[0, tp])]
    for c in loads:
        c.start()
    row = lax.rem(pc.y, tb_ref.shape[0])
    n_layers = tab_ref.shape[0]
    for l in range(n_layers):
        mod_ref[l, :6, :] = tab_ref[l].astype(F32) + tb_ref[row].astype(F32)
    for l in range(n_layers):
        mod_ref[l, 6:, :] = fin_ref[...].astype(F32) + te_ref[row].astype(F32) if l == n_layers - 1 else mod_ref[l + 1, :2, :]
    pc.barrier()
    tick(0)
    for c in loads:
        c.wait()
    kv_vm[0, n_cap:, :] = jnp.zeros((kv_vm.shape[1] - n_cap, kv_vm.shape[2]), BF)
    kv_vm[0, :n_cap, :] = dot_nt(cap_ref[...], wckv_vm[...]).astype(BF)
    load(0).wait()
    n0_vm[...] = norm_block(0)
    lax.fori_loop(0, tp // 2, pair_step, 0)
    attention(0)
    tokens(0, 13)
    load_w(1).start()
    own_copy().start()
    for i in range(3):
        pl.semaphore_wait(ready.at[i], 1)
    for i in "0312":
        ax(int(i)).start()
    ac(0).start()
    load_w(1).wait()
    lax.fori_loop(0, tp, gathered_step, 0)
    attention(1)
    for i in range(4):
        ax(i).wait_send()
        ac(i).wait_send()
    for d in range(2):
        af(d).wait_send()
    e = jnp.concatenate(tokens(1, 37), axis=1) + bo_ref[...].astype(F32).T
    n_rows, n_ch, width = eps_vm.shape[1:]
    n_pairs = n_rows // 2
    src = lax.broadcasted_iota(jnp.int32, (blk, n_pairs * width), 0)
    dst = lax.broadcasted_iota(jnp.int32, (blk, n_pairs * width), 1)
    spread = jnp.where(src == lax.shift_right_logical(dst, 1), 1.0, 0.0).astype(BF)
    hi = e.astype(BF)
    r1 = e - hi.astype(F32)
    mid = r1.astype(BF)
    lo = (r1 - mid.astype(F32)).astype(BF)
    wide = dot(hi, spread) + dot(mid, spread) + dot(lo, spread)
    odd = lax.rem(lax.broadcasted_iota(jnp.int32, (n_ch, width), 1), 2) == 1
    for i in range(n_pairs):
        for p in range(2):
            lanes = slice(i * width, (i + 1) * width)
            q0 = wide[4 * p * n_ch:(4 * p + 1) * n_ch, lanes]
            q1 = wide[(4 * p + 2) * n_ch:(4 * p + 3) * n_ch, lanes]
            eps_vm[pc.y, 2 * i + p] = jnp.where(odd, q1, q0)

    def e_copy(r):
        return copy_to(eps_vm.at[pc.y], eps_vm.at[pc.y], e_send.at[r], e_recv.at[r], cfg=lax.rem(pc.y + r, n_cfg))

    for r in range(1, n_cfg):
        e_copy(r).start()
    for r in range(1, n_cfg):
        e_copy(r).wait_recv()
    n_img = n_cfg // 2
    for b in range(n_img):
        ec, eu = eps_vm[b], eps_vm[n_img + b]
        guided = eu + GUIDANCE * (ec - eu)
        abar_t, abar_prev = al_ref[b:b + 1, :1], al_ref[b:b + 1, 1:]
        x0 = (xt_vm[b] - jnp.sqrt(1.0 - abar_t) * guided) / jnp.sqrt(abar_t)
        out_ref[b, mine] = jnp.sqrt(abar_prev) * x0 + jnp.sqrt(1.0 - abar_prev) * guided

    def r_copy(r):
        ref = out_ref.at[:, mine]
        return copy_to(ref, ref, e_send.at[n_cfg + r], e_recv.at[n_cfg + r], tp=lax.rem(pc.t + r, tp))

    for r in range(1, tp):
        r_copy(r).start()
    for r in range(1, tp):
        r_copy(r).wait_recv()
    for r in range(1, n_cfg):
        e_copy(r).wait_send()
    for r in range(1, tp):
        r_copy(r).wait_send()
    for key in gathers:
        gathers[key].finish()


def sampling_step(args, owns, tp, n_cfg, heads, hd):
    n_tok, dim = args[0].shape
    xt = args[10]
    blk, hw, kb = n_tok // tp, heads * hd, KEY_BLOCK
    dma = pltpu.SemaphoreType.DMA
    n_chunks = sum(len(p) for p in PLAN)
    n_layers = args[1].shape[0]
    kv = jax.ShapeDtypeStruct((-(-args[2].shape[0] // 16) * 16, args[3].shape[0]), BF)
    n_ff = tp * owns[3].shape[1]
    o_shape = (tp, heads, hd, blk)
    vmem = [
        ((n_layers, 8, dim), F32), ((3 * n_ff // 2, dim), BF), ((tp * hw, dim), BF), ((tp * hw, dim), BF), ((blk, dim), F32), ((blk, dim), BF), ((blk, n_ff), BF),
        ((tp * heads, hd, blk), BF), ((tp,) + kv.shape, BF), ((n_layers,) + o_shape, BF), (o_shape, BF),
        ((heads, n_tok, hw), BF), ((n_tok, hw), BF), ((heads, 80, n_tok), BF), ((max(kb, tp * hw), 2 * blk), F32), ((kb, 2 * blk), F32),
        ((n_cfg, xt.shape[1] // tp) + xt.shape[2:], F32), ((xt.shape[0], xt.shape[1] // tp) + xt.shape[2:], F32),
    ]
    res = pl.pallas_call(
        functools.partial(step_kernel, (tp, n_cfg, heads, hd, kb)),
        out_shape=[jax.ShapeDtypeStruct(xt.shape, F32)] + [chunk_shape(n[0], owns + (kv,), tp) for p in PLAN for n in p],
        in_specs=[HBM_SPEC] * 2 + [VMEM_SPEC, HBM_SPEC] + [VMEM_SPEC] * 6 + [HBM_SPEC, VMEM_SPEC, pl.BlockSpec(memory_space=pltpu.SMEM)] + [HBM_SPEC] * 5,
        out_specs=[VMEM_SPEC] + [HBM_SPEC] * n_chunks,
        scratch_shapes=[pltpu.VMEM(*v) for v in vmem] + [
            dma((tp,)), dma((8, 2 * tp)), dma((10,)), dma((10,)), dma((n_chunks * N_KIND,)), dma((n_chunks * N_KIND,)),
            dma((n_layers, tp)), dma((n_layers, tp)), dma((n_cfg + tp,)), dma((n_cfg + tp,)), pltpu.SemaphoreType.REGULAR((3,)),
        ],
        compiler_params=pltpu.CompilerParams(vmem_limit_bytes=67043328, collective_id=1, has_side_effects=True),
    )(*args, *owns)
    return res[0]


def solution(mesh):
    row_spec = P(('dp', 'cfg'))
    part_spec = P('dp')
    def tp_at(k):
        return P(*[None] * k, 'tp')

    in_specs = (row_spec,) * 3 + (part_spec,) * 4 + (P(), tp_at(3), tp_at(1), tp_at(2), tp_at(3), tp_at(1), tp_at(2), tp_at(1)) + (P(),) * 3
    tp = mesh.shape['tp']
    n_cfg = mesh.shape['cfg']

    def local_step(hidden, caption, cap_len, t_block, t_embed, x_t, alpha_bar, mod_table, w_qkv, w_proj, w_cq, w_ckv, w_cproj, w_fc1, w_fc2, final_table, w_out, b_out):
        dim = hidden.shape[2]
        n_layers, _, _, heads, hd = w_qkv.shape

        def rows_major(w, lead):
            return jnp.moveaxis(w, 1, -1).reshape(*lead, -1, dim)

        owns = (w_proj.reshape(n_layers, -1, dim), rows_major(w_cq, (n_layers,)), w_cproj.reshape(n_layers, -1, dim), w_fc1.mT, w_fc2)
        args = (hidden[0], rows_major(w_qkv, (n_layers,)), caption[0], rows_major(w_ckv, ()), mod_table, t_block.reshape(t_block.shape[0], -1, dim),
                t_embed[:, None], final_table, w_out.mT, b_out[None], x_t.mT, alpha_bar, cap_len)
        return sampling_step(args, owns, tp, n_cfg, heads, hd).mT

    return jax.shard_map(local_step, mesh=mesh, in_specs=in_specs, out_specs=part_spec, check_vma=False)
```

```python
import functools

import jax
import jax.numpy as jnp
from jax import lax
from jax.experimental import pallas as pl
from jax.experimental.pallas import tpu as pltpu
from jax.sharding import PartitionSpec as P

GUIDANCE = 4.5
LN_EPS = 1e-6
LOG2E = 1.4426950408889634
NT = (((1,), (1,)), ((), ()))
BF = jnp.bfloat16
F32 = jnp.float32
MESH = pl.DeviceIdType.MESH
VMEM_SPEC = pl.BlockSpec(memory_space=pltpu.VMEM)
HBM_SPEC = pl.BlockSpec(memory_space=pl.ANY)
N_KIND = 12
KEY_BLOCK = 512


def layer_norm(values):
    mean_val = jnp.mean(values, axis=-1, keepdims=True)
    centered = values - mean_val
    variance = jnp.mean(centered * centered, axis=-1, keepdims=True)
    return centered * lax.rsqrt(variance + LN_EPS)


def dot(a, b):
    return jnp.dot(a, b, preferred_element_type=F32)


def dot_nt(a, b):
    return lax.dot_general(a, b, NT, preferred_element_type=F32)


class Place:
    def __init__(self, tp, n_cfg):
        self.tp, self.n_cfg = tp, n_cfg
        self.t = lax.axis_index("tp")
        self.y = lax.axis_index("cfg")
        self.right = lax.rem(self.t + 2, tp)
        self.left = lax.rem(self.t + tp - 2, tp)
        self.far = lax.rem(self.t + 4, tp)
        self.mate = mate_of(self.t)
        self.up = lax.rem(self.y + 1, n_cfg)
        self.down = lax.rem(self.y + n_cfg - 1, n_cfg)
        same = (self.t, self.left, self.right, self.far)
        self.slots = same + tuple(mate_of(s) for s in same)

    def barrier(self):
        sem = pltpu.get_barrier_semaphore()
        for r in range(1, self.tp):
            pl.semaphore_signal(sem, inc=1, device_id={"tp": lax.rem(self.t + r, self.tp)}, device_id_type=MESH)
        for r in range(1, self.n_cfg):
            pl.semaphore_signal(sem, inc=1, device_id={"cfg": lax.rem(self.y + r, self.n_cfg)}, device_id_type=MESH)
        pl.semaphore_wait(sem, self.tp + self.n_cfg - 2)


def mate_of(t):
    return t + 1 - 2 * lax.rem(t, 2)


class Gather:
    def __init__(self, place, own, full, sems, sem_base, div):
        self.pc, self.own, self.full, self.sems, self.sem_base, self.div = place, own, full, sems, sem_base, div
        self.unit = own.shape[0] // div
        self.todo = [int(c) for c in {"1": "0125", "2": "01245", "4": "012345"}[str(div)]]
        self.p0 = (self.unit // 2 + 7) // 8 * 8
        self.p1 = self.unit - self.p0
        self.u = lax.rem(place.y, div)

    def copy(self, kind, src, dst, **dev):
        send, recv = self.sems
        return pltpu.make_async_remote_copy(src_ref=src, dst_ref=dst, send_sem=send.at[self.sem_base + kind],
                                            recv_sem=recv.at[self.sem_base + kind], device_id=dev, device_id_type=MESH)

    def part(self, unit, d):
        start = unit * self.unit
        if d is None:
            return pl.ds(pl.multiple_of(start, 8), self.unit)
        return pl.ds(pl.multiple_of(start + d * self.p0, 8), (self.p0, self.p1)[d])

    def x(self, d):
        rows = self.part(self.u, None)
        return self.copy(d, self.own.at[rows], self.full.at[1 + d, rows], tp=(self.pc.right, self.pc.left)[d])

    def f(self, d):
        pc = self.pc
        rows = self.part(self.u, d)
        return self.copy(2 + d, self.full.at[1 + d, rows], self.full.at[3, rows], tp=(pc.right, pc.left)[d])

    def v(self, far, d):
        ref = self.full.at[(pl.ds(1, 2), pl.ds(3, 1))[far], self.part(self.u, d if self.div == 2 else None)]
        return self.copy(4 + 2 * far + d, ref, ref, cfg=(self.pc.up, self.pc.down)[d])

    def w(self, d):
        unit = lax.rem(self.u + (self.div - 1, 1)[d], self.div)
        ref = self.full.at[pl.ds(1, 3), self.part(unit, d)]
        return self.copy(8 + d, ref, ref, cfg=(self.pc.up, self.pc.down)[d])

    def c(self, own):
        if own:
            return self.copy(11, self.own, self.full.at[4], tp=self.pc.mate)
        return self.copy(10, self.full.at[pl.ds(1, 3)], self.full.at[pl.ds(5, 3)], tp=self.pc.mate)

    def run(self, stage):
        ends = range(2)
        vert = ends if self.div > 1 else ()
        if stage == 0:
            for d in ends:
                self.x(d).start()
            self.c(True).start()
        elif stage == 1:
            for d in ends:
                self.x(d).wait_recv()
                self.f(d).start()
            for d in vert:
                self.v(0, d).start()
        elif stage == 2:
            for d in ends:
                self.f(d).wait_recv()
            for d in vert:
                self.v(1, d).start()
            if self.div == 1:
                self.c(False).start()
        elif stage == 3:
            for d in ends:
                self.v(0, d).wait_recv()
                self.v(1, d).wait_recv()
                self.w(d).start()
        elif stage == 4:
            for d in ends:
                if self.div == 4:
                    self.w(d).wait_recv()
                else:
                    self.v(0, d).wait_recv()
                    self.v(1, d).wait_recv()
            self.c(False).start()
        else:
            self.c(True).wait_recv()
            self.c(False).wait_recv()

    def advance(self):
        if self.todo:
            self.run(self.todo.pop(0))

    def require(self):
        while self.todo:
            self.advance()

    def finish(self):
        self.require()
        for d in range(2):
            self.x(d).wait_send()
            self.f(d).wait_send()
            if self.div > 1:
                self.v(0, d).wait_send()
                self.v(1, d).wait_send()
            if self.div == 4:
                self.w(d).wait_send()
        self.c(True).wait_send()
        self.c(False).wait_send()


def chunk_own(name, owns, layer):
    if name == "L":
        return owns[5]
    if name in "ABC":
        return owns["ABC".index(name)].at[layer]
    rows = owns[3].shape[1]
    if name in "DEFG":
        k, n = "DEFG".index(name), rows // 2
    else:
        k, n = "defghijk".index(name), rows // 4
    per = rows // n
    return owns[3 + k // per].at[layer, pl.ds(k % per * n, n)]


def chunk_shape(name, owns, tp):
    if name == "L":
        return jax.ShapeDtypeStruct((tp,) + owns[5].shape, BF)
    rows = owns[0].shape[1] if name in "ABC" else owns[3].shape[1] // (2 if name in "DEFG" else 4)
    return jax.ShapeDtypeStruct((tp, rows, owns[0].shape[2]), BF)


SLOTS = "0123456789abcdefghijklmnopqrstuvwxyzABCDEFGHIJKLMNOP"
PLAN = (
    ("C26adj", "B2346a", "F437bdf", "A2146b", "G2degi", "L126a", "E401237", "D4479ce"),
    ("F48hnqw", "C2finv", "A2fvwA", "E2twBE", "D4ciqtz", "G4hklnv", "B2hkty"),
)


def copy_to(src, dst, send_sem, recv_sem, **dev):
    return pltpu.make_async_remote_copy(src_ref=src, dst_ref=dst, send_sem=send_sem, recv_sem=recv_sem, device_id=dev, device_id_type=MESH)


def step_kernel(cfg, *refs):
    (tp, n_cfg, heads, hd, kb) = cfg
    hid_ref, wqkv_ref, cap_ref, wckv_ref, tab_ref, tb_ref, te_ref, fin_ref, wo_ref, bo_ref, xt_ref, al_ref, len_ref = refs[:13]
    owns = refs[13:18]
    out_ref = refs[18]
    pos = 19
    pc = Place(tp, n_cfg)
    n_chunks = sum(len(p) for p in PLAN)
    fulls = refs[pos:pos + n_chunks]
    (mod_ref, wbuf, wa, wcq, xres, a_vm, h_vm, qc_vm, kv_vm, o_in, o_vm, q_vm, k_vm, vt_vm, s0, s1, eps_vm, xt_vm,
     in_sems, w_sems, a_send, a_recv, g_send, g_recv, o_send, o_get, e_send, e_recv, ready) = refs[pos + n_chunks:]
    owns += (kv_vm.at[0],)
    gathers, starts = {}, {}
    for layer, chunks in enumerate(PLAN):
        for entry in chunks:
            i = len(gathers)
            gathers[layer, entry[0]] = Gather(pc, chunk_own(entry[0], owns, layer), fulls[i], (g_send, g_recv), i * N_KIND, int(entry[1]))
            starts[layer, entry[0]] = [SLOTS.index(c) for c in entry[2:]]

    def slot_events(slot):
        return [key for key, at in starts.items() if slot in at and len(gathers[key].todo) > 1]

    def tick(slot):
        for key in slot_events(slot):
            gathers[key].advance()

    def loop_ticks(i, base, count):
        for k in range(count):
            if slot_events(base + k):
                @pl.when(i == k)
                def _():
                    tick(base + k)

    n_tok, dim = hid_ref.shape
    blk = n_tok // tp
    hw = heads * hd
    scale = hd ** -0.5 * LOG2E
    part_rows = wbuf.shape[0] // 3
    part_of = [pl.ds(i * part_rows, part_rows) for i in range(3)]
    x_vm = wbuf.at[pl.ds(part_rows, n_tok)]
    n0_vm, n1_vm = wbuf.at[pl.ds(0, blk)], wbuf.at[pl.ds(blk, blk)]
    half = blk // 2
    halves = [slice(i * half, (i + 1) * half) for i in range(2)]

    def rows_of(i):
        return pl.ds(pl.multiple_of(i * blk, blk), blk)

    def load(i):
        return pltpu.make_async_copy(hid_ref.at[rows_of(i)], x_vm.at[rows_of(i)], in_sems.at[i])

    def load_w(layer):
        return pltpu.make_async_copy(wqkv_ref.at[layer], wcq.at[pl.ds(0, 3 * hw)], w_sems.at[7, tp + 1])

    def x_half(s, part):
        return x_vm.at[pl.ds(pl.multiple_of(s * blk + part * half, half), half)]

    def ax(i):
        d, part = i // 2, i % 2
        return copy_to(a_vm.at[pl.ds(part * half, half)], x_half(pc.t, part), a_send.at[i], a_recv.at[i], tp=(pc.right, pc.left)[d])

    def af(d):
        ref = x_half((pc.left, pc.right)[d], d)
        return copy_to(ref, ref, a_send.at[4 + d], a_recv.at[4 + d], tp=(pc.right, pc.left)[d])

    def ac(i):
        ref = x_vm.at[rows_of(pc.slots[i])]
        return copy_to(ref if i else a_vm, ref, a_send.at[6 + i], a_recv.at[6 + i], tp=pc.mate)

    def qkv_block(layer, i, x):
        rows = rows_of(i)
        qkv = dot_nt(x, wcq[:3 * hw, :])
        q = qkv[:, :hw] * scale
        lane = lax.broadcasted_iota(jnp.int32, q.shape, 1)
        for h in range(heads):
            q_vm[h, rows, :] = jnp.where((lane >= h * hd) & (lane < (h + 1) * hd), q, 0.0).astype(BF)
        k_vm[rows, :] = qkv[:, hw:2 * hw].astype(BF)
        vt = qkv[:, 2 * hw:].T
        for h in range(heads):
            vt_vm[h, :hd, rows] = vt[h * hd:(h + 1) * hd, :].astype(BF)

    def norm(x, layer, i):
        return (layer_norm(x) * (1.0 + mod_ref[layer, i + 1:i + 2, :]) + mod_ref[layer, i:i + 1, :]).astype(BF)

    def norm_block(i):
        return norm(x_vm[rows_of(i), :].astype(F32), 0, 0)

    def pair_step(i, carry):
        loop_ticks(i, 1, tp // 2)
        load(2 * i + 1).wait()
        n1_vm[...] = norm_block(2 * i + 1)
        qkv_block(0, 2 * i, n0_vm[...])

        @pl.when(2 * i + 2 < tp)
        def _():
            load(2 * i + 2).wait()

        n0_vm[...] = norm_block(jnp.minimum(2 * i + 2, tp - 1))
        qkv_block(0, 2 * i + 1, n1_vm[...])
        return carry

    def gathered_step(i, carry):
        b = pc.t
        for k, slot in enumerate("04125637"):
            b = jnp.where(i == k, pc.slots[int(slot)], b)

        def at(k, *acts):
            @pl.when(i == k)
            def _():
                for act in acts:
                    act()

        loop_ticks(i, 21, tp)
        at(0, own_copy().wait)
        at(1, ac(0).wait_recv)
        at(2, ax(0).wait_recv, af(0).start, ax(3).wait_recv, af(1).start, ax(1).wait_recv, ac(1).start)
        at(3, ax(2).wait_recv, ac(2).start)
        at(4, ac(1).wait_recv)
        at(5, ac(2).wait_recv)
        at(6, af(0).wait_recv, af(1).wait_recv, ac(3).start)
        at(7, ac(3).wait_recv)
        qkv_block(1, b, x_vm[rows_of(b), :])
        return carry

    def own_copy():
        return pltpu.make_async_copy(a_vm, x_vm.at[rows_of(pc.t)], in_sems.at[0])

    qb = 2 * blk
    qs = qb // 4
    n_q, n_kb = n_tok // qb, n_tok // kb
    bufs = (s0, s1)

    def o_copy(layer, dest, src):
        return copy_to(o_vm.at[dest], o_in.at[layer, src], o_send.at[layer, dest], o_get.at[layer, src], tp=dest)

    def o_local(layer):
        return pltpu.make_async_copy(o_vm.at[pc.t], o_in.at[layer, pc.t], in_sems.at[0])

    def q_block(k):
        return lax.rem(k + lax.div(pc.t, 2) + 1, n_q)

    def send_o(layer, k):
        for u in range(2):
            dest = q_block(k) * 2 + u

            @pl.when(dest != pc.t)
            def _():
                o_copy(layer, dest, pc.t).start()

            @pl.when(dest == pc.t)
            def _():
                o_local(layer).start()

    def q_step(layer, i, carry):
        h = lax.rem(i, heads)
        k = lax.div(i, heads)
        loop_ticks(i, (5, 29)[layer], heads * n_q)

        @pl.when((h == 0) & (k > 0))
        def _():
            send_o(layer, k - 1)

        qi = q_block(k)
        cols = range(4)

        def scores(j, c):
            q = q_vm[h, pl.ds(pl.multiple_of(qi * qb + c * qs, qs), qs), :]
            s = dot_nt(k_vm[j * kb:(j + 1) * kb, :], q)
            bufs[j % 2][:kb, c * qs:(c + 1) * qs] = s
            return jnp.max(jnp.max(s.reshape(kb // 8, 8, qs), axis=0), axis=0, keepdims=True)

        def weighted(j, c, m):
            pv = None
            for r in range(0, kb, qs):
                p = jnp.exp2(bufs[j % 2][r:r + qs, c * qs:(c + 1) * qs] - m).astype(BF)
                part = dot(vt_vm[h, :, j * kb + r:j * kb + r + qs], p)
                pv = part if pv is None else pv + part
            return pv

        m = [scores(0, c) for c in cols]
        acc = [None for c in cols]
        for j in range(n_kb):
            for c in cols:
                blk_max = scores(j + 1, c) if j + 1 < n_kb else None
                pv = weighted(j, c, m[c])
                acc[c] = pv if j == 0 else acc[c] + pv
                if blk_max is not None:
                    m_new = jnp.maximum(m[c], blk_max)
                    acc[c] = acc[c] * jnp.exp2(m[c] - m_new)
                    m[c] = m_new
        for c in cols:
            o = (acc[c][:hd] / acc[c][hd:hd + 1]).astype(BF)
            o_vm[qi * 2 + c // 2, h, :, (c % 2) * qs:(c % 2 + 1) * qs] = o
        return carry

    def attention(layer):
        lax.fori_loop(0, heads * n_q, functools.partial(q_step, layer), 0)
        send_o(layer, n_q - 1)
        for s in range(tp):
            @pl.when(s != pc.t)
            def _():
                o_copy(layer, s, s).wait_send()
                o_copy(layer, s, s).wait_recv()
        o_local(layer).wait()

    def pull(layer, which, part, dst):
        rows = owns[which].shape[1]
        n = rows // 2
        names = ("ABC"[which],) if which < 3 else ("DEFG"[2 * which - 6 + part],)
        if which > 2 and (layer, names[0]) not in gathers:
            i = 4 * which - 12 + 2 * part
            names = ("defghijk"[i], "defghijk"[i + 1])
        size = gathers[layer, names[0]].full.shape[1]
        res = []
        for k in range(tp):
            for u, name in enumerate(names):
                src = chunk_own(name, owns, layer) if k == 0 else gathers[layer, name].full.at[k]
                start = pc.slots[k] * size * len(names) + u * size
                res.append(pltpu.make_async_copy(src, dst.at[pl.ds(pl.multiple_of(start, 8), size)], w_sems.at[which + 2 * part, len(res)]))
        return [(layer, n) for n in names], res

    def fetch(*args):
        keys, copies = pull(*args)
        for key in keys:
            gathers[key].require()
        for c in copies:
            c.start()

    def ready_w(*args):
        for c in pull(*args)[1]:
            c.wait()

    def kv_copies():
        return [pltpu.make_async_copy(gathers[0, "L"].full.at[k], kv_vm.at[k], w_sems.at[7, k]) for k in range(1, tp)]

    def tokens(layer, base):
        loc = heads
        n_heads = tp * loc

        def mod(i):
            return mod_ref[layer, i:i + 1, :]

        fetch(layer, 0, 0, wa)
        fetch(layer, 1, 0, wcq)
        if layer == 0:
            gathers[0, "L"].require()
            for c in kv_copies():
                c.start()
        tick(base)
        ready_w(layer, 0, 0, wa)
        if layer == 0:
            x_load.wait()
        x1 = []
        for sl in halves:
            o = jnp.concatenate([o_in[layer, s, h, :, sl].astype(F32) for s in range(tp) for h in range(loc)], axis=0).T.astype(BF)
            x0 = a_vm[sl, :].astype(F32) if layer == 0 else xres[sl, :]
            x1.append(x0 + mod(2) * dot(o, wa[...]).astype(BF).astype(F32))
        fetch(layer, 2, 0, wa)
        w1_at, w2_at = (part_of[0], part_of[1]), (part_of[2], part_of[0])
        ready_w(layer, 1, 0, wcq)
        for i, sl in enumerate(halves):
            qt = (dot_nt(x1[i].astype(BF), wcq[...]) * scale).T
            for h in range(n_heads):
                qc_vm[h, :, sl] = qt[h * hd:(h + 1) * hd, :].astype(BF)
        tick(base + 1)
        if layer == 0:
            for c in kv_copies():
                c.wait()
        n_key = kv_vm.shape[1]
        ones = jnp.where(lax.broadcasted_iota(jnp.int32, (80 - hd, n_key), 0) == 0, 1.0, 0.0)
        lane0 = layer * 2 * hw
        key_bias = jnp.where(lax.broadcasted_iota(jnp.int32, (n_key, blk), 0) < jnp.minimum(len_ref[0], cap_ref.shape[0]), 0.0, -1e30)

        def cross_scores(n):
            k, h = n // loc, n % loc
            return dot(kv_vm[k, :, lane0 + h * hd:lane0 + (h + 1) * hd], qc_vm[pc.slots[k] * loc + h]) + key_bias

        s_next = cross_scores(0)
        for n in range(n_heads):
            k, h = n // loc, n % loc
            if n == tp:
                tick(base + 2)
            if h == 0:
                v_t = kv_vm[k, :, lane0 + hw:lane0 + 2 * hw].astype(F32).T
            s = s_next
            if n + 1 < n_heads:
                s_next = cross_scores(n + 1)
            p = jnp.exp2(s - jnp.max(s, axis=0, keepdims=True)).astype(BF)
            vt = jnp.concatenate([v_t[h * hd:(h + 1) * hd], ones], axis=0).astype(BF)
            pv = dot(vt, p)
            s0[pl.ds(pl.multiple_of((pc.slots[k] * loc + h) * hd, 8), hd), :blk] = (pv[:hd] / pv[hd:hd + 1]).astype(BF).astype(F32)
        tick(base + 3)
        fetch(layer, 3, 0, wbuf.at[w1_at[0]])
        ready_w(layer, 2, 0, wa)
        x2, a2 = [], []
        for i, sl in enumerate(halves):
            oc = s0[:, sl].T.astype(BF)
            x2.append(x1[i] + dot(oc, wa[...]).astype(BF).astype(F32))
            a2.append(norm(x2[i], layer, 3))
        tick(base + 4)
        fetch(layer, 4, 0, wbuf.at[w2_at[0]])
        step = part_rows // 2
        order = [(j, i) for j in range(4) for i in range(2)]

        def fc1(j, i):
            return dot_nt(a2[i], wbuf[j * step:(j + 1) * step, :])

        ready_w(layer, 3, 0, wbuf.at[w1_at[0]])
        h_next = fc1(*order[0])
        for n, (j, i) in enumerate(order):
            if (j, i) == (1, 0):
                fetch(layer, 3, 1, wbuf.at[w1_at[1]])
            if (j, i) == (1, 1):
                tick(base + 5)
                ready_w(layer, 3, 1, wbuf.at[w1_at[1]])
            hidden = h_next
            if n + 1 < len(order):
                h_next = fc1(*order[n + 1])
            h_vm[halves[i], j * step:(j + 1) * step] = jax.nn.gelu(hidden, approximate=True).astype(BF)
        tick(base + 6)
        fetch(layer, 4, 1, wbuf.at[w2_at[1]])
        ready_w(layer, 4, 0, wbuf.at[w2_at[0]])
        y = [dot(h_vm[sl, :part_rows], wbuf[w2_at[0], :]) for sl in halves]
        if layer == 0:
            for i, dev in enumerate((pc.left, pc.right, pc.mate)):
                pl.semaphore_signal(ready.at[i], inc=1, device_id={"tp": dev}, device_id_type=MESH)
        tick(base + 7)
        ready_w(layer, 4, 1, wbuf.at[w2_at[1]])
        res = []
        for i, sl in enumerate(halves):
            x3 = x2[i] + mod(5) * (y[i] + dot(h_vm[sl, part_rows:], wbuf[w2_at[1], :])).astype(BF).astype(F32)
            if layer == 0:
                xres[sl, :] = x3
                a_vm[sl, :] = norm(x3, layer, 6)
            else:
                res.append(dot_nt(wo_ref[...], norm(x3, layer, 6)))
        return res

    for i in range(tp):
        load(i).start()
    x_load = pltpu.make_async_copy(hid_ref.at[rows_of(pc.t)], a_vm, w_sems.at[7, tp])
    x_load.start()
    row_id = lax.broadcasted_iota(jnp.int32, (80 - hd, n_tok), 0)
    for h in range(heads):
        vt_vm[h, hd:, :] = jnp.where(row_id == 0, 1.0, 0.0).astype(BF)
    n_cap = cap_ref.shape[0]
    wckv_vm = wa.at[pl.ds(0, wckv_ref.shape[0])]
    n_rows = eps_vm.shape[1]
    mine = pl.ds(pc.t * n_rows, n_rows)
    loads = [load_w(0), pltpu.make_async_copy(xt_ref.at[:, mine], xt_vm, w_sems.at[1, tp]), pltpu.make_async_copy(wckv_ref, wckv_vm, w_sems.at[0, tp])]
    for c in loads:
        c.start()
    row = lax.rem(pc.y, te_ref.shape[0])
    n_mods, n_layers = tab_ref.shape[:2]

    def of_image(ref, lanes):
        res = ref[:1, lanes]
        for b in range(1, ref.shape[0]):
            res = jnp.where(row == b, ref[b:b + 1, lanes], res)
        return res.astype(F32)

    for i in range(n_mods):
        shared = of_image(tb_ref, slice(i * dim, (i + 1) * dim))
        for l in range(n_layers):
            mod_ref[l, i:i + 1, :] = tab_ref[i, l:l + 1, :].astype(F32) + shared
    for l in range(n_layers - 1):
        mod_ref[l, n_mods:, :] = mod_ref[l + 1, :2, :]
    mod_ref[n_layers - 1, n_mods:, :] = fin_ref[...].astype(F32) + of_image(te_ref, slice(0, dim))
    pc.barrier()
    tick(0)
    for c in loads:
        c.wait()
    kv_vm[0, n_cap:, :] = jnp.zeros((kv_vm.shape[1] - n_cap, kv_vm.shape[2]), BF)
    kv_vm[0, :n_cap, :] = dot_nt(cap_ref[...], wckv_vm[...]).astype(BF)
    load(0).wait()
    n0_vm[...] = norm_block(0)
    lax.fori_loop(0, tp // 2, pair_step, 0)
    attention(0)
    tokens(0, 13)
    load_w(1).start()
    own_copy().start()
    for i in range(3):
        pl.semaphore_wait(ready.at[i], 1)
    for i in "0312":
        ax(int(i)).start()
    ac(0).start()
    load_w(1).wait()
    lax.fori_loop(0, tp, gathered_step, 0)
    attention(1)
    for i in range(4):
        ax(i).wait_send()
        ac(i).wait_send()
    for d in range(2):
        af(d).wait_send()
    e = jnp.concatenate(tokens(1, 37), axis=1) + bo_ref[...].astype(F32).T
    n_rows, n_ch, width = eps_vm.shape[1:]
    n_pairs = n_rows // 2
    src = lax.broadcasted_iota(jnp.int32, (blk, n_pairs * width), 0)
    dst = lax.broadcasted_iota(jnp.int32, (blk, n_pairs * width), 1)
    spread = jnp.where(src == lax.shift_right_logical(dst, 1), 1.0, 0.0).astype(BF)
    hi = e.astype(BF)
    r1 = e - hi.astype(F32)
    mid = r1.astype(BF)
    lo = (r1 - mid.astype(F32)).astype(BF)
    wide = dot(hi, spread) + dot(mid, spread) + dot(lo, spread)
    odd = lax.rem(lax.broadcasted_iota(jnp.int32, (n_ch, width), 1), 2) == 1
    for i in range(n_pairs):
        for p in range(2):
            lanes = slice(i * width, (i + 1) * width)
            q0 = wide[4 * p * n_ch:(4 * p + 1) * n_ch, lanes]
            q1 = wide[(4 * p + 2) * n_ch:(4 * p + 3) * n_ch, lanes]
            eps_vm[pc.y, 2 * i + p] = jnp.where(odd, q1, q0)

    def e_copy(r):
        return copy_to(eps_vm.at[pc.y], eps_vm.at[pc.y], e_send.at[r], e_recv.at[r], cfg=lax.rem(pc.y + r, n_cfg))

    for r in range(1, n_cfg):
        e_copy(r).start()
    for r in range(1, n_cfg):
        e_copy(r).wait_recv()
    n_img = n_cfg // 2
    for b in range(n_img):
        ec, eu = eps_vm[b], eps_vm[n_img + b]
        guided = eu + GUIDANCE * (ec - eu)
        abar_t, abar_prev = al_ref[b:b + 1, :1], al_ref[b:b + 1, 1:]
        x0 = (xt_vm[b] - jnp.sqrt(1.0 - abar_t) * guided) / jnp.sqrt(abar_t)
        out_ref[b, mine] = jnp.sqrt(abar_prev) * x0 + jnp.sqrt(1.0 - abar_prev) * guided

    def r_copy(r):
        ref = out_ref.at[:, mine]
        return copy_to(ref, ref, e_send.at[n_cfg + r], e_recv.at[n_cfg + r], tp=lax.rem(pc.t + r, tp))

    for r in range(1, tp):
        r_copy(r).start()
    for r in range(1, tp):
        r_copy(r).wait_recv()
    for r in range(1, n_cfg):
        e_copy(r).wait_send()
    for r in range(1, tp):
        r_copy(r).wait_send()
    for key in gathers:
        gathers[key].finish()


def sampling_step(args, owns, tp, n_cfg, heads, hd):
    n_tok, dim = args[0].shape
    xt = args[10]
    blk, hw, kb = n_tok // tp, heads * hd, KEY_BLOCK
    dma = pltpu.SemaphoreType.DMA
    n_chunks = sum(len(p) for p in PLAN)
    n_layers = args[1].shape[0]
    kv = jax.ShapeDtypeStruct((-(-args[2].shape[0] // 16) * 16, args[3].shape[0]), BF)
    n_ff = tp * owns[3].shape[1]
    o_shape = (tp, heads, hd, blk)
    vmem = [
        ((n_layers, 8, dim), F32), ((3 * n_ff // 2, dim), BF), ((tp * hw, dim), BF), ((tp * hw, dim), BF), ((blk, dim), F32), ((blk, dim), BF), ((blk, n_ff), BF),
        ((tp * heads, hd, blk), BF), ((tp,) + kv.shape, BF), ((n_layers,) + o_shape, BF), (o_shape, BF),
        ((heads, n_tok, hw), BF), ((n_tok, hw), BF), ((heads, 80, n_tok), BF), ((max(kb, tp * hw), 2 * blk), F32), ((kb, 2 * blk), F32),
        ((n_cfg, xt.shape[1] // tp) + xt.shape[2:], F32), ((xt.shape[0], xt.shape[1] // tp) + xt.shape[2:], F32),
    ]
    res = pl.pallas_call(
        functools.partial(step_kernel, (tp, n_cfg, heads, hd, kb)),
        out_shape=[jax.ShapeDtypeStruct(xt.shape, F32)] + [chunk_shape(n[0], owns + (kv,), tp) for p in PLAN for n in p],
        in_specs=[HBM_SPEC] * 2 + [VMEM_SPEC, HBM_SPEC] + [VMEM_SPEC] * 6 + [HBM_SPEC, VMEM_SPEC, pl.BlockSpec(memory_space=pltpu.SMEM)] + [HBM_SPEC] * 5,
        out_specs=[VMEM_SPEC] + [HBM_SPEC] * n_chunks,
        scratch_shapes=[pltpu.VMEM(*v) for v in vmem] + [
            dma((tp,)), dma((8, 2 * tp)), dma((10,)), dma((10,)), dma((n_chunks * N_KIND,)), dma((n_chunks * N_KIND,)),
            dma((n_layers, tp)), dma((n_layers, tp)), dma((n_cfg + tp,)), dma((n_cfg + tp,)), pltpu.SemaphoreType.REGULAR((3,)),
        ],
        compiler_params=pltpu.CompilerParams(vmem_limit_bytes=67043328, collective_id=1, has_side_effects=True),
    )(*args, *owns)
    return res[0]


def solution(mesh):
    row_spec = P(('dp', 'cfg'))
    part_spec = P('dp')
    def tp_at(k):
        return P(*[None] * k, 'tp')

    in_specs = (row_spec,) * 3 + (part_spec,) * 4 + (P(), tp_at(3), tp_at(1), tp_at(2), tp_at(3), tp_at(1), tp_at(2), tp_at(1)) + (P(),) * 3
    tp = mesh.shape['tp']
    n_cfg = mesh.shape['cfg']

    def local_step(hidden, caption, cap_len, t_block, t_embed, x_t, alpha_bar, mod_table, w_qkv, w_proj, w_cq, w_ckv, w_cproj, w_fc1, w_fc2, final_table, w_out, b_out):
        dim = hidden.shape[2]
        n_layers, _, _, heads, hd = w_qkv.shape

        def rows_major(w, lead):
            return jnp.moveaxis(w, 1, -1).reshape(*lead, -1, dim)

        owns = (w_proj.reshape(n_layers, -1, dim), rows_major(w_cq, (n_layers,)), w_cproj.reshape(n_layers, -1, dim), w_fc1.mT, w_fc2)
        args = (hidden[0], rows_major(w_qkv, (n_layers,)), caption[0], rows_major(w_ckv, ()), jnp.swapaxes(mod_table, 0, 1), t_block,
                t_embed, final_table, w_out.mT, b_out[None], x_t.mT, alpha_bar, cap_len)
        return sampling_step(args, owns, tp, n_cfg, heads, hd).mT

    return jax.shard_map(local_step, mesh=mesh, in_specs=in_specs, out_specs=part_spec, check_vma=False)
```
